128 devices in a mesh: dp: 32 (over x, z_hi, y), expert: 4 (over z_lo, core).
Axes of the slice: x: 4, y: 4, z: 4 (z_hi: 2, z_lo: 2; z = z_hi * 2 + z_lo), core: 2. Of those that a mesh axis runs over, the one named last changes fastest.
Arguments:
- tokens: bfloat16 [16384, 2048], P(('dp', 'expert')), may hold values from -6 to 6
- cotangent: bfloat16 [16384, 2048], P(('dp', 'expert')), may hold values from -6 to 6
- expert_ids: int32 [16384, 2], P(('dp', 'expert')), may hold values from 0 to 3, all different within a row; in each aligned block of 128 rows (0 to 127, 128 to 255, ...) at most 128 rows name the same one
- combine: float32 [16384, 2], P(('dp', 'expert')), may hold values from 0.1 to 1
- w_gate: bfloat16 [4, 2048, 768], P('expert'), may hold values from -0.125 to 0.125
- w_up: bfloat16 [4, 2048, 768], P('expert'), may hold values from -0.125 to 0.125
- w_down: bfloat16 [4, 768, 2048], P('expert'), may hold values from -0.21875 to 0.21875
Outputs:
- input_grad: bfloat16 [16384, 2048], P(('dp', 'expert'))
- combine_grad: float32 [16384, 2], P(('dp', 'expert'))
- gate_grad: bfloat16 [4, 2048, 768], P('expert', 'dp')
- up_grad: bfloat16 [4, 2048, 768], P('expert', 'dp')
- down_grad: bfloat16 [4, 768, 2048], P('expert', 'dp')
The draws below stay inside these ranges and needn't reach their ends.
Inputs may be any that keep to these rules, and one draw needn't show every extreme that they name: `expert_ids`: each token names 2 different experts. In the rows of one device no expert is named by more than 128 tokens, and in some devices' rows some expert is named by exactly 128.
All inputs are finite; a program needn't handle non-finite values.
Results may differ from the reference program's by a relative error of at most 0.02.
Values may be sent and summed in bfloat16 or wider, within the bound.
No kernel may reach another device: no remote copies, remote signals or barrier semaphores. Data moves between devices by JAX's collectives and lax.ppermute only.
A program may use at most 128 MiB of HBM per device.

```python
import math
import jax
import jax.numpy as jnp
import numpy as np
from jax import lax

D = 2048
FF = 768
TOK_DEV = 128
TOP = 2
EXPERTS = 4
CAP = 128
TOKENS = 16384
N_DP = 32
N_EXPERT = 4


def steps_of(own_key, shape, split, smallest, largest):
    gain, own = 1.0, jax.random.fold_in(own_key, 6)
    for axis_at, parts in split:
        heights = jnp.exp(jax.random.uniform(jax.random.fold_in(own, axis_at), (parts,), jnp.float32, smallest / len(split), largest / len(split)))
        gain = gain * jnp.repeat(heights, shape[axis_at] // parts).reshape([-1 if axis == axis_at else 1 for axis in range(len(shape))])
    return gain


def deal_out(own_key, own, number, rows, number_of, top, bound, skew):
    ranking = jax.random.permutation(own_key, number_of)
    crowded, common = load_shares(number_of, rows * top, bound, skew, True), load_shares(number_of, rows * top, bound, skew, False)
    places = jnp.arange(number_of)

    def named(lengths, offset_by):
        used = int((lengths > 0).sum())
        fixed = max(1, used // 4)
        shifted = fixed + (places - fixed + offset_by * (used - fixed)) % max(1, number_of - fixed)
        return jnp.zeros((number_of,), jnp.int32).at[ranking[jnp.where(places < fixed, places, shifted)]].set(jnp.asarray(lengths, jnp.int32))

    lengths = jnp.where(number % 4 == 0, named(crowded, number // 4), named(common, number - number // 4 - 1))
    mixed = jax.random.permutation(jax.random.fold_in(own, 3), number_of)
    donor, taker = mixed[0:number_of // 2 * 2:2], mixed[1:number_of // 2 * 2:2]
    room = jnp.minimum(lengths[donor] - 1, bound - lengths[taker]) // 2
    room = jnp.where((donor == ranking[0]) | (taker == ranking[0]) | (lengths[taker] == 0), 0, jnp.maximum(room, 0))
    shifted = jax.random.randint(jax.random.fold_in(own, 4), (number_of // 2,), 0, 1 << 20) % (room + 1)
    lengths = lengths.at[donor].add(-shifted).at[taker].add(shifted)
    items = jnp.searchsorted(jnp.cumsum(lengths), jnp.arange(rows * top), side="right").astype(jnp.int32)
    listing = items.reshape(top, rows).T
    listing = listing[jax.random.permutation(jax.random.fold_in(own, 1), rows)]
    offset_by = jax.random.randint(jax.random.fold_in(own, 2), (rows, 1), 0, top)
    return jnp.take_along_axis(listing, (jnp.arange(top)[None, :] + offset_by) % top, axis=1)


def load_shares(number_of, total, bound, skew, full):
    weights = [(1 << 20) // math.isqrt(standing ** skew) + 1 for standing in range(1, number_of + 1)]
    largest = bound if full else min(bound, max(-(-total // number_of), total * weights[0] // sum(weights)))
    least = 1 if total - largest >= number_of - 1 else 0
    holding, spare = [largest] + [least] * (number_of - 1), total - largest - least * (number_of - 1)
    while spare > 0:
        candidates = [i for i in range(1, number_of) if holding[i] < largest] or [i for i in range(1, number_of) if holding[i] < bound]
        mass, left = sum([weights[i] for i in candidates]), spare
        for i in candidates:
            more = min(bound - holding[i], max(1, left * weights[i] // mass), spare)
            holding[i] = holding[i] + more
            spare = spare - more
    return np.array(holding)


def noise(rng, shape, deviation, reach, split=(), kind=jnp.bfloat16):
    result = jax.random.normal(rng, shape, jnp.float32) * deviation
    if len(split) > 0:
        result = steps_of(rng, shape, split, -0.22, 0.18) * result
    return jnp.clip(result, min=-reach, max=reach).astype(kind)


def setup_inputs(seed: int = 0) -> dict:
    key_list = jax.random.split(jax.random.key(seed), 8)
    tokens = noise(key_list[0], (TOKENS, D), 1.0, 6.0, ((0, 128),))
    cotangent = noise(key_list[1], (TOKENS, D), 1.0, 6.0, ((0, 128),))
    expert_ids_keys = jax.random.split(jax.random.fold_in(key_list[2], 1), TOKENS // TOK_DEV)
    expert_ids_turns = jax.random.permutation(jax.random.fold_in(key_list[2], 3), TOKENS // TOK_DEV)
    expert_ids = jax.vmap(lambda own, number: deal_out(jax.random.fold_in(key_list[2], 2), own, number, TOK_DEV, EXPERTS, TOP, CAP, 2))(expert_ids_keys, expert_ids_turns).reshape((TOKENS, TOP))
    combine = jnp.clip(jnp.exp(math.log(1.0) - 2.3025851 * jax.random.uniform(key_list[3], (TOKENS, TOP), jnp.float32) ** steps_of(key_list[3], (TOKENS, TOP), ((0, 128),), -0.2, 0.2)), 0.1, 1.0)
    w_gate = noise(key_list[4], (EXPERTS, D, FF), D ** -0.5, 0.125, ((0, 4),))
    w_up = noise(key_list[5], (EXPERTS, D, FF), D ** -0.5, 0.125, ((0, 4),))
    w_down = noise(key_list[6], (EXPERTS, FF, D), FF ** -0.5, 0.21875, ((0, 4),))
    return dict(tokens=tokens, cotangent=cotangent, expert_ids=expert_ids, combine=combine, w_gate=w_gate, w_up=w_up, w_down=w_down)


def slot_table(expert_ids, experts_all, capacity):
    pairs = expert_ids.reshape(-1).astype(jnp.int32)
    count = pairs.shape[0]
    onehot = (pairs[:, None] == jnp.arange(experts_all, dtype=jnp.int32)[None, :]).astype(jnp.int32)
    before = jnp.cumsum(onehot, axis=0) - onehot
    position = jnp.sum(before * onehot, axis=1).astype(jnp.int32)
    dest = (pairs * capacity + position).astype(jnp.int32)
    filled = jnp.zeros((experts_all * capacity,), jnp.int32).at[dest].set(jnp.arange(count, dtype=jnp.int32) + 1)
    return dest, filled


def gather_rows(tokens, cotangent, combine, filled, top):
    live = filled > 0
    pair = jnp.maximum(filled - 1, 0).astype(jnp.int32)
    source = (pair // top).astype(jnp.int32)
    rows_x = jnp.where(live[:, None], jnp.take(tokens, source, axis=0), jnp.zeros((), tokens.dtype))
    rows_dy = jnp.where(live[:, None], jnp.take(cotangent, source, axis=0), jnp.zeros((), cotangent.dtype))
    rows_c = jnp.where(live, jnp.take(combine.reshape(-1), pair, axis=0), jnp.zeros((), combine.dtype))
    return rows_x, rows_dy, rows_c


def forward_part(rows_x, gate_mat, up_mat, down_mat):
    gate = jnp.dot(rows_x, gate_mat, preferred_element_type=jnp.float32)
    up = jnp.dot(rows_x, up_mat, preferred_element_type=jnp.float32)
    sig = jax.nn.sigmoid(gate)
    act = gate * sig
    hidden = (act * up).astype(jnp.bfloat16)
    output = jnp.dot(hidden, down_mat, preferred_element_type=jnp.float32)
    return gate, up, sig, act, hidden, output


def backward_part(state, rows_dy, rows_c, gate_mat, up_mat, down_mat):
    gate, up, sig, act, hidden, output = state
    comb_grad = jnp.sum(rows_dy.astype(jnp.float32) * output, axis=1)
    scaled = (rows_c[:, None] * rows_dy.astype(jnp.float32)).astype(jnp.bfloat16)
    last = (((1,), (1,)), ((), ()))
    hidden_grad = lax.dot_general(scaled, down_mat, last, preferred_element_type=jnp.float32)
    gate_d = (hidden_grad * up * (sig * (1.0 + gate * (1.0 - sig)))).astype(jnp.bfloat16)
    up_d = (hidden_grad * act).astype(jnp.bfloat16)
    row_grad = lax.dot_general(gate_d, gate_mat, last, preferred_element_type=jnp.float32)
    row_grad = (row_grad + lax.dot_general(up_d, up_mat, last, preferred_element_type=jnp.float32)).astype(jnp.bfloat16)
    return comb_grad, scaled, gate_d, up_d, row_grad


def reference(tokens, cotangent, expert_ids, combine, w_gate, w_up, w_down):
    first = (((0,), (0,)), ((), ()))
    x_all = tokens.reshape(N_DP, N_EXPERT, TOK_DEV, D)
    dy_all = cotangent.reshape(N_DP, N_EXPERT, TOK_DEV, D)
    id_all = expert_ids.reshape(N_DP, N_EXPERT, TOK_DEV, TOP)
    c_all = combine.reshape(N_DP, N_EXPERT, TOK_DEV, TOP)

    def prepare(x_q, dy_q, id_q, c_q):
        dest, filled = slot_table(id_q, EXPERTS, CAP)
        rows_x, rows_dy, rows_c = gather_rows(x_q, dy_q, c_q, filled, TOP)
        return dest, rows_x.reshape(EXPERTS, CAP, D), rows_dy.reshape(EXPERTS, CAP, D), rows_c.reshape(EXPERTS, CAP)

    def one_expert(item):
        inputs, cot_rows, comb_rows, gate_mat, up_mat, down_mat = item
        state = forward_part(inputs, gate_mat, up_mat, down_mat)
        comb_grad, scaled, gate_d, up_d, row_grad = backward_part(state, cot_rows, comb_rows, gate_mat, up_mat, down_mat)
        gate_part = lax.dot_general(inputs, gate_d, first, preferred_element_type=jnp.float32).astype(jnp.bfloat16)
        up_part = lax.dot_general(inputs, up_d, first, preferred_element_type=jnp.float32).astype(jnp.bfloat16)
        down_part = lax.dot_general(state[4], scaled, first, preferred_element_type=jnp.float32).astype(jnp.bfloat16)
        return row_grad, comb_grad, gate_part, up_part, down_part

    def finish(flat_rows, flat_comb, dest):
        picked = jnp.take(flat_rows, dest, axis=0).reshape(TOK_DEV, TOP, D)
        summed = jnp.sum(picked.astype(jnp.float32), axis=1).astype(jnp.bfloat16)
        return summed, jnp.take(flat_comb, dest, axis=0).reshape(TOK_DEV, TOP)

    def one_replica(carry, inputs):
        x_r, dy_r, id_r, c_r = inputs
        dest, rx, rdy, rc = jax.vmap(prepare)(x_r, dy_r, id_r, c_r)
        group_x = jnp.transpose(rx, (1, 0, 2, 3)).reshape(EXPERTS, N_EXPERT * CAP, D)
        group_dy = jnp.transpose(rdy, (1, 0, 2, 3)).reshape(EXPERTS, N_EXPERT * CAP, D)
        group_c = jnp.transpose(rc, (1, 0, 2)).reshape(EXPERTS, N_EXPERT * CAP)
        rows, combs, gate_part, up_part, down_part = lax.map(one_expert, (group_x, group_dy, group_c, w_gate, w_up, w_down))
        gate_part, up_part, down_part = lax.optimization_barrier((gate_part, up_part, down_part))
        carry = (carry[0] + gate_part.astype(jnp.float32), carry[1] + up_part.astype(jnp.float32), carry[2] + down_part.astype(jnp.float32))
        back = jnp.transpose(rows.reshape(EXPERTS, N_EXPERT, CAP, D), (1, 0, 2, 3)).reshape(N_EXPERT, EXPERTS * CAP, D)
        back_c = jnp.transpose(combs.reshape(EXPERTS, N_EXPERT, CAP), (1, 0, 2)).reshape(N_EXPERT, EXPERTS * CAP)
        grads_in, grads_c = jax.vmap(finish)(back, back_c, dest)
        return carry, (grads_in, grads_c)

    start = (jnp.zeros((EXPERTS, D, FF), jnp.float32), jnp.zeros((EXPERTS, D, FF), jnp.float32), jnp.zeros((EXPERTS, FF, D), jnp.float32))
    sums, (grads_in, grads_c) = lax.scan(one_replica, start, (x_all, dy_all, id_all, c_all))
    input_grad = grads_in.reshape(TOKENS, D)
    combine_grad = grads_c.reshape(TOKENS, TOP)
    return (input_grad, combine_grad, sums[0].astype(jnp.bfloat16), sums[1].astype(jnp.bfloat16), sums[2].astype(jnp.bfloat16))
```

```python
import functools

import jax
import jax.numpy as jnp
import numpy as np
from jax import lax
from jax.experimental import pallas as pl
from jax.experimental.pallas import tpu as pltpu
from jax.sharding import Mesh
from jax.sharding import PartitionSpec as P


F32 = jnp.float32
BF16 = jnp.bfloat16
GROUP = ("zl", "c")
REPLICA = ("x", "zh", "y")
EVERY = ("x", "zh", "y", "zl", "c")
XA, XB, YA, YB, Z = ("x", 1), ("x", 3), ("y", 1), ("y", 3), ("zh", 1)
ORDERS = ((XA, YA, XB, YB, Z), (YA, XB, YB, XA, Z), (XB, YB, XA, YA, Z), (YB, XA, YA, XB, Z))
BLOCKS = 32
COLS = 2


def moved(array, axis, mask):
    return lax.ppermute(array, axis, [(i, i ^ mask) for i in range(lax.axis_size(axis))])


def block_table():
    masks = np.zeros((3, len(ORDERS), BLOCKS), np.int32)
    for p, order in enumerate(ORDERS):
        for pos in range(BLOCKS):
            for step, (axis, mask) in enumerate(order):
                if pos >> (4 - step) & 1:
                    masks[REPLICA.index(axis), p, pos] ^= mask
    x, z, y = (lax.axis_index(axis) ^ jnp.asarray(m) for axis, m in zip(REPLICA, masks))
    return ((x * 2 + z) * 4 + y).astype(jnp.int32)


def nt(a, b):
    return lax.dot_general(a, b, (((1,), (1,)), ((), ())), preferred_element_type=F32)


def nn(a, b):
    return jnp.dot(a, b, preferred_element_type=F32)


def whole(shape):
    return pl.BlockSpec(shape, lambda *_: (0,) * len(shape))


def params():
    return pltpu.CompilerParams(vmem_limit_bytes=56 * 1024 * 1024)


def forward_body(x0, x1, x2, x3, cw, wg, wu, slope, act_out, hid, cht, xt, xs):
    @pl.when(pl.program_id(0) == 0)
    def _():
        for j, x in enumerate((x0, x1, x2, x3)):
            xs[pl.ds(j * 128, 128), :] = x[...]
        xt[...] = xs[...].T

    gate = nn(xs[...], wg[...])
    up = nn(xs[...], wu[...])
    sig = jax.nn.sigmoid(gate)
    act = gate * sig
    slope[...] = up * (sig * (1.0 + gate * (1.0 - sig)))
    act_out[...] = act
    hidden = act * up
    hid[...] = hidden.astype(BF16)
    cht[...] = (cw[...] * hidden).T


def forward(pieces, cw, wg, wu):
    d, ff = wg.shape
    rows, tile = 4 * pieces[0].shape[0], 256
    wide = pl.BlockSpec((d, tile), lambda f: (0, f))
    tall = pl.BlockSpec((rows, tile), lambda f: (0, f))
    return pl.pallas_call(
        forward_body,
        grid=(ff // tile,),
        in_specs=[whole(p.shape) for p in pieces] + [whole(cw.shape), wide, wide],
        out_specs=[tall, tall, tall, pl.BlockSpec((tile, rows), lambda f: (f, 0)), whole((d, rows))],
        out_shape=[
            jax.ShapeDtypeStruct((rows, ff), F32),
            jax.ShapeDtypeStruct((rows, ff), F32),
            jax.ShapeDtypeStruct((rows, ff), BF16),
            jax.ShapeDtypeStruct((ff, rows), F32),
            jax.ShapeDtypeStruct((d, rows), BF16),
        ],
        scratch_shapes=[pltpu.VMEM((rows, d), BF16)],
        compiler_params=params(),
        cost_estimate=pl.CostEstimate(flops=4 * rows * d * ff, transcendentals=0, bytes_accessed=12 << 20),
        name="forward",
    )(*pieces, cw, wg, wu)


def down_body(p, idx, cht, g0, g1, g2, g3, send, keep, mixed, gs):
    for j, g in enumerate((g0, g1, g2, g3)):
        gs[pl.ds(j * 128, 128), :] = g[...]
    size = cht.shape[0] // BLOCKS
    for pos in range(BLOCKS):
        start = pl.multiple_of(idx[p, pos] * size, 8)
        mixed[pl.ds(pos * size, size), :] = cht[pl.ds(start, size), :]
    half = cht.shape[0] // 2
    send[...] = nn(mixed[pl.ds(half, half), :].astype(BF16), gs[...]).astype(BF16)
    keep[...] = nn(mixed[pl.ds(0, half), :].astype(BF16), gs[...]).astype(BF16)


def down_part(p, idx, cht, chunks):
    ff, rows = cht.shape
    cols = 512
    per = 4 // COLS
    pieces = chunks[p // per]
    spec = pl.BlockSpec((128, cols), lambda *_: (0, p % per))
    return pl.pallas_call(
        functools.partial(down_body, p),
        grid=(1,),
        in_specs=[pl.BlockSpec(memory_space=pltpu.SMEM), whole(cht.shape)] + [spec] * 4,
        out_specs=[whole((ff // 2, cols))] * 2,
        out_shape=[jax.ShapeDtypeStruct((ff // 2, cols), BF16)] * 2,
        scratch_shapes=[pltpu.VMEM((ff, rows), F32), pltpu.VMEM((rows, cols), BF16)],
        compiler_params=params(),
        cost_estimate=pl.CostEstimate(flops=2 * rows * cols * ff, transcendentals=0, bytes_accessed=4 << 20),
        name=f"down{p}",
    )(idx, cht, *pieces)


def hidden_body(*refs):
    pieces = refs[: 4 * COLS]
    cw, wd, slope, act, hid, gd, ud, comb, gs = refs[4 * COLS :]
    width = gs.shape[1] // COLS

    @pl.when(pl.program_id(0) == 0)
    def _():
        for k in range(COLS):
            for j in range(4):
                gs[pl.ds(j * 128, 128), pl.ds(k * width, width)] = pieces[k * 4 + j][...]
        comb[...] = jnp.zeros_like(comb)

    back = nt(gs[...], wd[...])
    comb[...] += jnp.sum(hid[...].astype(F32) * back, axis=1, keepdims=True)
    back = cw[...] * back
    gd[...] = (back * slope[...]).astype(BF16)
    ud[...] = (back * act[...]).astype(BF16)


def hidden_part(chunks, cw, wd, slope, act, hid):
    ff, d = wd.shape
    rows, tile = slope.shape[0], 256
    tall = pl.BlockSpec((rows, tile), lambda f: (0, f))
    flat = [g for chunk in chunks for g in chunk]
    return pl.pallas_call(
        hidden_body,
        grid=(ff // tile,),
        in_specs=[whole(g.shape) for g in flat]
        + [whole(cw.shape), pl.BlockSpec((tile, d), lambda f: (f, 0)), tall, tall, tall],
        out_specs=[tall, tall, whole((rows, 1))],
        out_shape=[
            jax.ShapeDtypeStruct((rows, ff), BF16),
            jax.ShapeDtypeStruct((rows, ff), BF16),
            jax.ShapeDtypeStruct((rows, 1), F32),
        ],
        scratch_shapes=[pltpu.VMEM((rows, d), BF16)],
        compiler_params=params(),
        cost_estimate=pl.CostEstimate(flops=2 * rows * d * ff, transcendentals=0, bytes_accessed=8 << 20),
        name="hidden",
    )(*flat, cw, wd, slope, act, hid)


def gate_body(p, idx, xt, gd, send, keep, mixed):
    size = xt.shape[0] // BLOCKS
    for pos in range(BLOCKS):
        start = pl.multiple_of(idx[p, pos] * size, size)
        mixed[pl.ds(pos * size, size), :] = xt[pl.ds(start, size), :]
    half = xt.shape[0] // 2
    send[...] = nn(mixed[pl.ds(half, half), :], gd[...]).astype(BF16)
    keep[...] = nn(mixed[pl.ds(0, half), :], gd[...]).astype(BF16)


def gate_part(p, idx, xt, grad):
    d, rows = xt.shape
    cols = grad.shape[1] // 2
    return pl.pallas_call(
        functools.partial(gate_body, p),
        grid=(1,),
        in_specs=[
            pl.BlockSpec(memory_space=pltpu.SMEM),
            whole(xt.shape),
            pl.BlockSpec((rows, cols), lambda *_: (0, p % 2)),
        ],
        out_specs=[whole((d // 2, cols))] * 2,
        out_shape=[jax.ShapeDtypeStruct((d // 2, cols), BF16)] * 2,
        scratch_shapes=[pltpu.VMEM((d, rows), BF16)],
        compiler_params=params(),
        cost_estimate=pl.CostEstimate(flops=2 * rows * cols * d, transcendentals=0, bytes_accessed=6 << 20),
        name=f"gate{p}",
    )(idx, xt, grad)


def rows_body(gd, ud, wg, wu, r0, r1, r2, r3):
    total = (nt(gd[...], wg[...]) + nt(ud[...], wu[...])).astype(BF16)
    for j, r in enumerate((r0, r1, r2, r3)):
        r[...] = total[j * 128 : (j + 1) * 128, :]


def rows_part(gd, ud, wg, wu):
    d, ff = wg.shape
    rows, tile = gd.shape[0], 512
    weight = pl.BlockSpec((tile, ff), lambda n: (n, 0))
    return pl.pallas_call(
        rows_body,
        grid=(d // tile,),
        in_specs=[whole(gd.shape), whole(ud.shape), weight, weight],
        out_specs=[pl.BlockSpec((rows // 4, tile), lambda n: (0, n))] * 4,
        out_shape=[jax.ShapeDtypeStruct((rows // 4, d), BF16)] * 4,
        compiler_params=params(),
        cost_estimate=pl.CostEstimate(flops=4 * rows * d * ff, transcendentals=0, bytes_accessed=10 << 20),
        name="rows",
    )(gd, ud, wg, wu)


def added(arrays, start, stop):
    return sum(a[start:stop].astype(F32) for a in arrays).astype(BF16)


def chain(order, send, keep):
    have, left = [keep], keep.shape[0]
    for axis, mask in order[:-1]:
        have.append(moved(send, axis, mask))
        send = added(have, left // 2, left)
        left //= 2
    have.append(moved(send, *order[-1]))
    return added(have, 0, left)


def shards(tokens, cotangent, expert_ids, combine, w_gate, w_up, w_down):
    wg, wu, wd = w_gate[0], w_up[0], w_down[0]
    width = cotangent.shape[1] // COLS
    mine = lax.axis_index(GROUP)
    idx = block_table()

    def gathered(own):
        across = moved(own, "zl", 1)
        return (own, moved(own, "c", 1), across, moved(across, "c", 1))

    def weights_for(mask):
        chosen = expert_ids == (mine ^ mask)
        return jnp.sum(jnp.where(chosen, combine, 0.0), axis=1)

    pieces = gathered(tokens)
    weights = [weights_for(0)] + [moved(weights_for(m), GROUP, m) for m in (1, 2, 3)]
    cw = jnp.concatenate(weights).reshape(-1, 1)
    chunks = [gathered(cotangent[:, k * width : (k + 1) * width]) for k in range(COLS)]

    slope, act, hid, cht, xt = forward(pieces, cw, wg, wu)
    down = [chain(ORDERS[p], *down_part(p, idx, cht, chunks)) for p in range(4)]
    gd, ud, comb = hidden_part(chunks, cw, wd, slope, act, hid)
    gates = [chain(ORDERS[p], *gate_part(p, idx, xt, gd if p < 2 else ud)) for p in range(4)]
    rows = rows_part(gd, ud, wg, wu)

    near = moved(rows[1], "c", 1)
    far = (rows[2].astype(F32) + moved(rows[3], "c", 1).astype(F32)).astype(BF16)
    far = moved(far, "zl", 1)
    input_grad = (rows[0].astype(F32) + near.astype(F32) + far.astype(F32)).astype(BF16)

    comb = comb.reshape(4, -1)
    given = [comb[0]] + [moved(comb[m], GROUP, m) for m in (1, 2, 3)]
    combine_grad = sum(
        jnp.where(expert_ids == (mine ^ m), given[m][:, None], 0.0) for m in range(4)
    )
    gate_grad = jnp.concatenate(gates[:2], axis=1)[None]
    up_grad = jnp.concatenate(gates[2:], axis=1)[None]
    down_grad = jnp.concatenate(down, axis=1)[None]
    return (input_grad, combine_grad, gate_grad, up_grad, down_grad)


def solution(mesh):
    torus = Mesh(mesh.devices.reshape(4, 2, 4, 2, 2), EVERY)
    tokens, weights, grads = P(EVERY, None), P(GROUP, None, None), P(GROUP, REPLICA, None)
    return jax.shard_map(
        shards,
        mesh=torus,
        in_specs=(tokens, tokens, tokens, tokens, weights, weights, weights),
        out_specs=(tokens, tokens, grads, grads, grads),
        check_vma=False,
    )
```

```python
import jax
import jax.numpy as jnp
import numpy as np
from jax import lax
from jax.experimental import pallas as pl
from jax.experimental.pallas import tpu as pltpu
from jax.sharding import Mesh
from jax.sharding import PartitionSpec as P


F32 = jnp.float32
BF16 = jnp.bfloat16
GROUP = ("zl", "c")
REPLICA = ("x", "zh", "y")
EVERY = ("x", "zh", "y", "zl", "c")
XA, XB, YA, YB, Z = ("x", 1), ("x", 3), ("y", 1), ("y", 3), ("zh", 1)
ORDERS = ((XA, XB, YA, YB, Z), (YA, YB, XA, XB, Z), (XB, XA, YB, YA, Z), (YB, YA, XB, XA, Z))
BLOCKS = 32
HALF = BLOCKS // 2
PIECE = 128
LANES = 128


def moved(array, axis, mask):
    return lax.ppermute(array, axis, [(i, i ^ mask) for i in range(lax.axis_size(axis))])


def block_table():
    masks = np.zeros((3, len(ORDERS), BLOCKS), np.int32)
    for p, order in enumerate(ORDERS):
        for pos in range(BLOCKS):
            for step, (axis, mask) in enumerate(order):
                if pos >> (4 - step) & 1:
                    masks[REPLICA.index(axis), p, pos] ^= mask
    x, z, y = (lax.axis_index(axis) ^ jnp.asarray(m) for axis, m in zip(REPLICA, masks))
    return ((x * 2 + z) * 4 + y).astype(jnp.int32)


def nt(a, b):
    return lax.dot_general(a, b, (((1,), (1,)), ((), ())), preferred_element_type=F32)


def nn(a, b):
    return jnp.dot(a, b, preferred_element_type=F32)


def kernel(body, ins, outs, limit, flops, smem=0, scratch=()):
    vmem = pl.BlockSpec(memory_space=pltpu.VMEM)
    return pl.pallas_call(
        body,
        in_specs=[pl.BlockSpec(memory_space=pltpu.SMEM)] * smem + [vmem] * (len(ins) - smem),
        out_specs=[vmem] * len(outs),
        out_shape=[jax.ShapeDtypeStruct(s, t) for s, t in outs],
        scratch_shapes=list(scratch),
        compiler_params=pltpu.CompilerParams(vmem_limit_bytes=limit << 20),
        cost_estimate=pl.CostEstimate(flops=flops, transcendentals=0, bytes_accessed=1 << 20),
    )(*ins)


def forward_body(x0, x1, x2, x3, cw, wg, wu, slope, act_out, hid, cht, xt, xs):
    for j, x in enumerate((x0, x1, x2, x3)):
        xs[pl.ds(j * PIECE, PIECE), :] = x[...]
    tile = 256
    for f in range(wg.shape[1] // tile):
        at = pl.ds(f * tile, tile)
        gate = nn(xs[...], wg[:, at])
        up = nn(xs[...], wu[:, at])
        sig = jax.nn.sigmoid(gate)
        act = gate * sig
        slope[:, at] = up * (sig * (1.0 + gate * (1.0 - sig)))
        act_out[:, at] = act
        hidden = act * up
        hid[:, at] = hidden.astype(BF16)
        cht[at, :] = (cw[...] * hidden).T
    for j in range(4):
        xt[:, pl.ds(j * PIECE, PIECE)] = xs[pl.ds(j * PIECE, PIECE), :].T


def down_body(first, idx, cht, g0, g1, g2, g3, *refs):
    outs, (mixed, gs) = refs[:4], refs[4:]
    for j, g in enumerate((g0, g1, g2, g3)):
        gs[pl.ds(j * PIECE, PIECE), :] = g[...]
    size = cht.shape[0] // BLOCKS
    cols = gs.shape[1] // 4
    for p in range(4):
        for b in range(HALF):
            start = pl.multiple_of(idx[p, first + b] * size, 8)
            mixed[p, pl.ds(b * size, size), :] = cht[pl.ds(start, size), :]
        part = nn(mixed[p].astype(BF16), gs[:, pl.ds(p * cols, cols)])
        for b in range(HALF):
            rows = part[b * size : (b + 1) * size]
            stack = [rows[:, k * LANES : (k + 1) * LANES] for k in range(cols // LANES)]
            tall = size * len(stack)
            outs[p][pl.ds(b * tall, tall), :] = jnp.concatenate(stack, axis=0).astype(BF16)


def down_half(first, idx, cht, pieces):
    ff, rows = cht.shape
    d = pieces[0].shape[1]
    out = ((HALF * ff // BLOCKS * (d // 4 // LANES), LANES), BF16)

    def body(*refs):
        down_body(first, *refs)

    return kernel(
        body,
        (idx, cht, *pieces),
        [out] * 4,
        16,
        rows * ff * d,
        smem=1,
        scratch=(pltpu.VMEM((4, ff // 2, rows), F32), pltpu.VMEM((rows, d), BF16)),
    )


def hidden_body(g0, g1, g2, g3, cw, wd, slope, act, hid, gd, ud, comb, gs):
    for j, g in enumerate((g0, g1, g2, g3)):
        gs[pl.ds(j * PIECE, PIECE), :] = g[...]
    tile = 256
    total = jnp.zeros(comb.shape, F32)
    for f in range(wd.shape[0] // tile):
        at = pl.ds(f * tile, tile)
        back = nt(gs[...], wd[at, :])
        total = total + jnp.sum(hid[:, at].astype(F32) * back, axis=1, keepdims=True)
        back = cw[...] * back
        gd[:, at] = (back * slope[:, at]).astype(BF16)
        ud[:, at] = (back * act[:, at]).astype(BF16)
    comb[...] = total


def gate_body(first, idx, xt, gd, ud, *refs):
    outs, mixed = refs[:4], refs[4]
    size = xt.shape[0] // BLOCKS // 2
    for p in range(4):
        for b in range(HALF):
            start = pl.multiple_of(idx[p, first + b] * (2 * size) + (p % 2) * size, size)
            mixed[p, pl.ds(b * size, size), :] = xt[pl.ds(start, size), :]
        grad = gd if p < 2 else ud
        cols = grad.shape[1]
        tile = 256
        per = tile // LANES
        tall = size * (cols // LANES)
        for n in range(cols // tile):
            part = nn(mixed[p], grad[:, pl.ds(n * tile, tile)]).astype(BF16)
            for b in range(HALF):
                for k in range(per):
                    at = b * tall + (n * per + k) * size
                    outs[p][pl.ds(at, size), :] = part[b * size : (b + 1) * size, k * LANES : (k + 1) * LANES]


def gate_half(first, idx, xt, gd, ud):
    d, rows = xt.shape
    ff = gd.shape[1]
    out = ((HALF * (d // BLOCKS // 2) * (ff // LANES), LANES), BF16)

    def body(*refs):
        gate_body(first, *refs)

    return kernel(
        body,
        (idx, xt, gd, ud),
        [out] * 4,
        12,
        2 * rows * ff * d,
        smem=1,
        scratch=(pltpu.VMEM((4, d // 4, rows), BF16),),
    )


def rows_body(gd, ud, wg, wu, r0, r1, r2, r3):
    tile = 512
    for n in range(wg.shape[0] // tile):
        at = pl.ds(n * tile, tile)
        total = (nt(gd[...], wg[at, :]) + nt(ud[...], wu[at, :])).astype(BF16)
        for j, r in enumerate((r0, r1, r2, r3)):
            r[:, at] = total[j * PIECE : (j + 1) * PIECE, :]


def summed(arrays, start, stop):
    total = 0.0
    for blocks, a in arrays:
        size = a.shape[0] // blocks
        total = total + a[start * size : stop * size].astype(F32)
    return total.astype(BF16)


def shards(tokens, cotangent, expert_ids, combine, w_gate, w_up, w_down):
    wg, wu, wd = w_gate[0], w_up[0], w_down[0]
    d, ff = wg.shape
    rows = 4 * PIECE
    mine = lax.axis_index(GROUP)
    idx = block_table()

    def gathered(own):
        across = moved(own, "zl", 1)
        beside = moved(own, "c", 1)
        return (own, beside, across, moved(across, "c", 1))

    def weights_for(mask):
        chosen = expert_ids == (mine ^ mask)
        return jnp.sum(jnp.where(chosen, combine, 0.0), axis=1)

    weights = [weights_for(0)] + [moved(weights_for(m), GROUP, m) for m in (1, 2, 3)]
    cw = jnp.concatenate(weights).reshape(-1, 1)
    xs = gathered(tokens)
    gs = gathered(cotangent)

    slope, act, hid, cht, xt = kernel(
        forward_body,
        (*xs, cw, wg, wu),
        [((rows, ff), F32), ((rows, ff), F32), ((rows, ff), BF16), ((ff, rows), F32), ((d, rows), BF16)],
        16,
        4 * rows * d * ff,
        scratch=(pltpu.VMEM((rows, d), BF16),),
    )
    down_send = down_half(HALF, idx, cht, gs)
    gd, ud, comb = kernel(
        hidden_body,
        (*gs, cw, wd, slope, act, hid),
        [((rows, ff), BF16), ((rows, ff), BF16), ((rows, 1), F32)],
        12,
        2 * rows * d * ff,
        scratch=(pltpu.VMEM((rows, d), BF16),),
    )
    gate_send = gate_half(HALF, idx, xt, gd, ud)
    down_keep = down_half(0, idx, cht, gs)
    gate_keep = gate_half(0, idx, xt, gd, ud)
    grads = kernel(rows_body, (gd, ud, wg, wu), [((PIECE, d), BF16)] * 4, 12, 4 * rows * d * ff)

    have = []
    for p, order in enumerate(ORDERS):
        pair = []
        for send, keep in ((down_send[p], down_keep[p]), (gate_send[p], gate_keep[p])):
            held = [(HALF, keep), (HALF, moved(send, *order[0]))]
            held.append((8, moved(summed(held, 8, 16), *order[1])))
            pair.append(held)
        have.append(pair)

    def joined(p, start, stop):
        return jnp.concatenate([summed(held, start, stop) for held in have[p]], axis=0)

    def shared(array, p, blocks):
        at = 0
        for held in have[p]:
            size = held[0][1].shape[0] // HALF * blocks
            held.append((blocks, array[at : at + size]))
            at += size

    for step, left in ((2, 8), (3, 4)):
        for p, order in enumerate(ORDERS):
            shared(moved(joined(p, left // 2, left), *order[step]), p, left // 2)
    last = jnp.concatenate([joined(p, 1, 2) for p in range(4)], axis=0)
    last = moved(last, *Z)
    share = last.shape[0] // 4
    for p in range(4):
        shared(last[p * share : (p + 1) * share], p, 1)
    down, gates = ([summed(have[p][k], 0, 1) for p in range(4)] for k in (0, 1))

    near = moved(grads[1], "c", 1)
    far = (grads[2].astype(F32) + moved(grads[3], "c", 1).astype(F32)).astype(BF16)
    far = moved(far, "zl", 1)
    input_grad = (grads[0].astype(F32) + near.astype(F32) + far.astype(F32)).astype(BF16)

    comb = comb.reshape(4, -1)
    given = [comb[0]] + [moved(comb[m], GROUP, m) for m in (1, 2, 3)]
    combine_grad = sum(
        jnp.where(expert_ids == (mine ^ m), given[m][:, None], 0.0) for m in range(4)
    )

    def side_by_side(part, height):
        return part.reshape(-1, height, LANES).transpose(1, 0, 2).reshape(height, -1)

    half = d // BLOCKS // 2
    gate_grad = jnp.concatenate([side_by_side(g, half) for g in gates[:2]], axis=0)[None]
    up_grad = jnp.concatenate([side_by_side(g, half) for g in gates[2:]], axis=0)[None]
    down_grad = jnp.concatenate([side_by_side(g, ff // BLOCKS) for g in down], axis=1)[None]
    return (input_grad, combine_grad, gate_grad, up_grad, down_grad)


def solution(mesh):
    torus = Mesh(mesh.devices.reshape(4, 2, 4, 2, 2), EVERY)
    tokens, weights, grads = P(EVERY, None), P(GROUP, None, None), P(GROUP, REPLICA, None)

    return jax.shard_map(
        shards,
        mesh=torus,
        in_specs=(tokens, tokens, tokens, tokens, weights, weights, weights),
        out_specs=(tokens, tokens, grads, grads, grads),
        check_vma=False,
    )
```

```python
import jax
import jax.numpy as jnp
from jax import lax
from jax.experimental import pallas as pl
from jax.experimental.pallas import tpu as pltpu
from jax.sharding import Mesh
from jax.sharding import PartitionSpec as P


F32 = jnp.float32
BF16 = jnp.bfloat16
GROUP = ("zl", "c")
REPLICA = ("x", "zh", "y")
EVERY = ("x", "zh", "y", "zl", "c")
XA, XB, YA, YB, Z = ("x", 1), ("x", 3), ("y", 1), ("y", 3), ("zh", 1)
ORDERS = ((XA, XB, YA, YB, Z), (YA, YB, XA, XB, Z), (XB, XA, YB, YA, Z), (YB, YA, XB, XA, Z))
DOWN_ORDERS = ORDERS[:2] + ((Z, XA, YB, YA, XB), (Z, YA, XB, XA, YB))
BLOCKS = 32
HALF = BLOCKS // 2
PIECE = 128
LANES = 128
ROW = ((8, LANES), F32)


def moved(array, axis, mask):
    return lax.ppermute(array, axis, [(i, i ^ mask) for i in range(lax.axis_size(axis))])


def block_at(order, pos):
    masks = dict.fromkeys(REPLICA, 0)
    for step, (axis, mask) in enumerate(order):
        if pos >> (4 - step) & 1:
            masks[axis] ^= mask
    x, z, y = (lax.axis_index(axis) ^ masks[axis] for axis in REPLICA)
    return (x * 2 + z) * 4 + y


def group_index():
    return lax.axis_index("zl") * 2 + lax.axis_index("c")


def as_row(column):
    return jnp.broadcast_to(column, (column.shape[0], LANES)).T[:8]


def as_column(row):
    return jnp.broadcast_to(row[0:1, :], (LANES, LANES)).T[:, 0:1]


def nt(a, b):
    return lax.dot_general(a, b, (((1,), (1,)), ((), ())), preferred_element_type=F32)


def nn(a, b):
    return jnp.dot(a, b, preferred_element_type=F32)


def kernel(body, ins, outs, limit, flops, scratch=()):
    vmem = pl.BlockSpec(memory_space=pltpu.VMEM)
    return pl.pallas_call(
        body,
        in_specs=[vmem] * len(ins),
        out_specs=[vmem] * len(outs),
        out_shape=[jax.ShapeDtypeStruct(s, t) for s, t in outs],
        scratch_shapes=list(scratch),
        compiler_params=pltpu.CompilerParams(vmem_limit_bytes=limit << 20),
        cost_estimate=pl.CostEstimate(flops=flops, transcendentals=0, bytes_accessed=1 << 20),
    )(*ins)


def route_body(ids, combine, *outs):
    mine = group_index()
    for m, out in enumerate(outs):
        chosen = ids[...] == (mine ^ m)
        row = jnp.sum(jnp.where(chosen, combine[...], 0.0), axis=0, keepdims=True)
        out[...] = jnp.broadcast_to(row, out.shape)


def combine_body(ids, c0, c1, c2, c3, out):
    mine = group_index()
    total = jnp.zeros(out.shape, F32)
    for m, c in enumerate((c0, c1, c2, c3)):
        total = total + jnp.where(ids[...] == (mine ^ m), c[0:1, :], 0.0)
    out[...] = total


def forward_body(x0, x1, c0, c1, wg, wu, slope, act_out, hid, cht, xt, xs):
    cw = jnp.concatenate([as_column(c0[...]), as_column(c1[...])], axis=0)
    for j, x in enumerate((x0, x1)):
        xs[pl.ds(j * PIECE, PIECE), :] = x[...]
    tile = 256
    for f in range(wg.shape[1] // tile):
        at = pl.ds(f * tile, tile)
        gate = nn(xs[...], wg[:, at])
        up = nn(xs[...], wu[:, at])
        sig = jax.nn.sigmoid(gate)
        act = gate * sig
        slope[:, at] = up * (sig * (1.0 + gate * (1.0 - sig)))
        act_out[:, at] = act
        hidden = act * up
        hid[:, at] = hidden.astype(BF16)
        cht[at, :] = (cw * hidden).T
    for j in range(2):
        xt[:, pl.ds(j * PIECE, PIECE)] = xs[pl.ds(j * PIECE, PIECE), :].T


def forward(x0, x1, cws, wg, wu):
    d, ff = wg.shape
    rows = 2 * PIECE
    outs = [((rows, ff), F32), ((rows, ff), F32), ((rows, ff), BF16), ((ff, rows), F32), ((d, rows), BF16)]
    return kernel(
        forward_body,
        (x0, x1, *cws, wg, wu),
        outs,
        12,
        4 * rows * d * ff,
        scratch=(pltpu.VMEM((rows, d), BF16),),
    )


def down_body(first, chunk, hta, htb, g0, g1, g2, g3, *refs):
    outs, (mixed, gs) = refs[:-2], refs[-2:]
    cols = g2.shape[1] // 2
    for j, g in enumerate((g0, g1)):
        gs[pl.ds(j * PIECE, PIECE), :] = g[:, pl.ds(chunk * 2 * cols, 2 * cols)]
    for j, g in enumerate((g2, g3)):
        gs[pl.ds((2 + j) * PIECE, PIECE), :] = g[...]
    size = hta.shape[0] // BLOCKS
    rows = hta.shape[1]
    for q in range(2):
        out = outs[q % len(outs)]
        base = q * (out.shape[0] // 2) if len(outs) == 1 else 0
        for b in range(HALF):
            start = pl.multiple_of(block_at(DOWN_ORDERS[2 * chunk + q], first + b) * size, 8)
            mixed[q, pl.ds(b * size, size), pl.ds(0, rows)] = hta[pl.ds(start, size), :]
            mixed[q, pl.ds(b * size, size), pl.ds(rows, rows)] = htb[pl.ds(start, size), :]
        part = nn(mixed[q].astype(BF16), gs[:, pl.ds(q * cols, cols)])
        for b in range(HALF):
            block = part[b * size : (b + 1) * size]
            stack = [block[:, k * LANES : (k + 1) * LANES] for k in range(cols // LANES)]
            tall = size * len(stack)
            out[pl.ds(base + b * tall, tall), :] = jnp.concatenate(stack, axis=0).astype(BF16)


def down_half(first, chunk, hts, pieces, joint=False):
    ff, rows = hts[0].shape
    width = pieces[2].shape[1]
    count = 1 if joint else 2
    out = ((2 // count * HALF * ff // BLOCKS * (width // 2 // LANES), LANES), BF16)

    def body(*refs):
        down_body(first, chunk, *refs)

    return kernel(
        body,
        (*hts, *pieces),
        [out] * count,
        12,
        2 * rows * ff * width,
        scratch=(pltpu.VMEM((2, ff // 2, 2 * rows), F32), pltpu.VMEM((2 * rows, width), BF16)),
    )


def hidden_body(pieces, c0, c1, wd, slope, act, hid, gd, ud, comb0, comb1, gs):
    cw = jnp.concatenate([as_column(c0[...]), as_column(c1[...])], axis=0)
    for j, chunks in enumerate(pieces):
        at = 0
        for g in chunks:
            gs[pl.ds(j * PIECE, PIECE), pl.ds(at, g.shape[1])] = g[...]
            at += g.shape[1]
    tile = 256
    total = jnp.zeros((gs.shape[0], 1), F32)
    for f in range(wd.shape[0] // tile):
        at = pl.ds(f * tile, tile)
        back = nt(gs[...], wd[at, :])
        total = total + jnp.sum(hid[:, at].astype(F32) * back, axis=1, keepdims=True)
        back = cw * back
        gd[:, at] = (back * slope[:, at]).astype(BF16)
        ud[:, at] = (back * act[:, at]).astype(BF16)
    comb0[...] = as_row(total[:PIECE])
    comb1[...] = as_row(total[PIECE:])


def hidden_part(pieces, cws, wd, slope, act, hid):
    ff, d = wd.shape
    rows = 2 * PIECE
    counts = [len(chunks) for chunks in pieces]

    def body(*refs):
        first, second = refs[: counts[0]], refs[counts[0] : sum(counts)]
        hidden_body((first, second), *refs[sum(counts) :])

    return kernel(
        body,
        (*pieces[0], *pieces[1], *cws, wd, slope, act, hid),
        [((rows, ff), BF16), ((rows, ff), BF16), ROW, ROW],
        10,
        2 * rows * d * ff,
        scratch=(pltpu.VMEM((rows, d), BF16),),
    )


def gate_body(first, xta, xtb, gda, gdb, uda, udb, *refs):
    outs, mixed = refs[:4], refs[4]
    size = xta.shape[0] // BLOCKS // 2
    rows = xta.shape[1]
    for p in range(4):
        for b in range(HALF):
            start = pl.multiple_of(block_at(ORDERS[p], first + b) * (2 * size) + (p % 2) * size, size)
            mixed[p, pl.ds(b * size, size), pl.ds(0, rows)] = xta[pl.ds(start, size), :]
            mixed[p, pl.ds(b * size, size), pl.ds(rows, rows)] = xtb[pl.ds(start, size), :]
        ga, gb = (gda, gdb) if p < 2 else (uda, udb)
        cols = ga.shape[1]
        tile = 256
        per = tile // LANES
        tall = size * (cols // LANES)
        for n in range(cols // tile):
            at = pl.ds(n * tile, tile)
            part = nn(mixed[p, :, pl.ds(0, rows)], ga[:, at]) + nn(mixed[p, :, pl.ds(rows, rows)], gb[:, at])
            part = part.astype(BF16)
            for b in range(HALF):
                for k in range(per):
                    to = b * tall + (n * per + k) * size
                    outs[p][pl.ds(to, size), :] = part[b * size : (b + 1) * size, k * LANES : (k + 1) * LANES]


def gate_half(first, xts, gds, uds):
    d, rows = xts[0].shape
    ff = gds[0].shape[1]
    out = ((HALF * (d // BLOCKS // 2) * (ff // LANES), LANES), BF16)

    def body(*refs):
        gate_body(first, *refs)

    return kernel(
        body,
        (*xts, *gds, *uds),
        [out] * 4,
        12,
        4 * rows * ff * d,
        scratch=(pltpu.VMEM((4, d // 4, 2 * rows), BF16),),
    )


def rows_body(gda, gdb, uda, udb, wg, wu, r0, r1, r2, r3, gd, ud):
    half = gda.shape[0]
    for scratch, pair in ((gd, (gda, gdb)), (ud, (uda, udb))):
        for j, ref in enumerate(pair):
            scratch[pl.ds(j * half, half), :] = ref[...]
    tile = 512
    for n in range(wg.shape[0] // tile):
        at = pl.ds(n * tile, tile)
        total = (nt(gd[...], wg[at, :]) + nt(ud[...], wu[at, :])).astype(BF16)
        for j, r in enumerate((r0, r1, r2, r3)):
            r[:, at] = total[j * PIECE : (j + 1) * PIECE, :]


def finish_body(base, last, end2, end3, gate, up, down):
    recv = [r[...].astype(F32) for r in (last, end2, end3)]
    total = base[...] + jnp.concatenate(recv, axis=0)
    half, low = gate.shape[0] // 2, down.shape[0]
    cols = down.shape[1] // 4
    at = 0
    for p in range(4):
        out = gate if p < 2 else up
        for k in range(gate.shape[1] // LANES):
            block = total[at : at + half].astype(BF16)
            out[pl.ds(p % 2 * half, half), pl.ds(k * LANES, LANES)] = block
            at += half
    for p in range(4):
        for k in range(cols // LANES):
            block = total[at : at + low].astype(BF16)
            down[:, pl.ds(p * cols + k * LANES, LANES)] = block
            at += low


def summed(arrays, start, stop, kind=BF16):
    total = 0.0
    for blocks, a in arrays:
        size = a.shape[0] // blocks
        total = total + a[start * size : stop * size].astype(F32)
    return total.astype(kind)


def shards(tokens, cotangent, expert_ids, combine, w_gate, w_up, w_down):
    wg, wu, wd = w_gate[0], w_up[0], w_down[0]
    d, ff = wg.shape
    rows = 4 * PIECE

    tok_far = moved(tokens, "zl", 1)
    tok_near = moved(tokens, "c", 1)
    own = kernel(route_body, (expert_ids.T, combine.T), [ROW] * 4, 2, 1 << 10)
    cws = [own[0]] + [moved(own[m], GROUP, m) for m in (1, 2, 3)]
    cwa, cwb = cws[:2], cws[2:]
    cot_near = moved(cotangent, "c", 1)
    cot_far = [moved(cotangent[:, k * d // 2 : (k + 1) * d // 2], "zl", 1) for k in range(2)]
    tok_both = moved(tok_far, "c", 1)
    cot_both = [moved(cot_far[k], "c", 1) for k in range(2)]

    fa = forward(tokens, tok_near, cwa, wg, wu)
    fb = forward(tok_far, tok_both, cwb, wg, wu)
    hts, xts = (fa[3], fb[3]), (fa[4], fb[4])
    pieces = [(cotangent, cot_near, cot_far[k], cot_both[k]) for k in range(2)]
    down_send = down_half(HALF, 0, hts, pieces[0])
    down_z = down_half(HALF, 1, hts, pieces[1], joint=True)[0]
    ha = hidden_part(((cotangent,), (cot_near,)), cwa, wd, *fa[:3])
    hb = hidden_part((cot_far, cot_both), cwb, wd, *fb[:3])
    gds, uds = (ha[0], hb[0]), (ha[1], hb[1])
    gate_send = gate_half(HALF, xts, gds, uds)
    down_keep = [a for k in range(2) for a in down_half(0, k, hts, pieces[k])]
    gate_keep = gate_half(0, xts, gds, uds)
    grads = kernel(
        rows_body,
        (*gds, *uds, wg, wu),
        [((PIECE, d), BF16)] * 4,
        12,
        4 * rows * d * ff,
        scratch=(pltpu.VMEM((rows, ff), BF16),) * 2,
    )

    down_z = moved(down_z, *Z)
    size = down_z.shape[0] // 2
    down_got = [moved(down_send[p], *ORDERS[p][0]) for p in (0, 1)]
    down_got += [lax.optimization_barrier(a) for a in (down_z[:size], down_z[size:])]
    have = [
        [
            [(HALF, gate_keep[p]), (HALF, moved(gate_send[p], *ORDERS[p][0]))],
            [(HALF, down_keep[p]), (HALF, down_got[p])],
        ]
        for p in range(4)
    ]

    def joined(p, start, stop, kind=BF16):
        return jnp.concatenate([summed(held, start, stop, kind) for held in have[p]], axis=0)

    def shared(array, p, blocks):
        at = 0
        for held in have[p]:
            size = held[0][1].shape[0] // HALF * blocks
            held.append((blocks, array[at : at + size]))
            at += size

    for step, left in ((1, 16), (2, 8), (3, 4)):
        for p in range(4):
            shared(moved(joined(p, left // 2, left), *ORDERS[p][step]), p, left // 2)
    gates, downs = ([have[p][k] for p in range(4)] for k in (0, 1))
    last = moved(jnp.concatenate([summed(h, 1, 2) for h in gates + downs[:2]], axis=0), *Z)
    others = [moved(summed(downs[p], 1, 2), *DOWN_ORDERS[p][4]) for p in (2, 3)]
    base = jnp.concatenate([summed(h, 0, 1, F32) for h in gates + downs], axis=0)
    gate_grad, up_grad, down_grad = kernel(
        finish_body,
        (base, last, *others),
        [((d // BLOCKS, ff), BF16), ((d // BLOCKS, ff), BF16), ((ff // BLOCKS, d), BF16)],
        4,
        1 << 20,
    )

    near = moved(grads[1], "c", 1)
    far = (grads[2].astype(F32) + moved(grads[3], "c", 1).astype(F32)).astype(BF16)
    far = moved(far, "zl", 1)
    input_grad = (grads[0].astype(F32) + near.astype(F32) + far.astype(F32)).astype(BF16)

    comb = [ha[2], ha[3], hb[2], hb[3]]
    given = [comb[0]] + [moved(comb[m], GROUP, m) for m in (1, 2, 3)]
    combine_grad = kernel(combine_body, (expert_ids.T, *given), [((2, PIECE), F32)], 2, 1 << 10)[0].T
    return (input_grad, combine_grad, gate_grad[None], up_grad[None], down_grad[None])


def solution(mesh):
    torus = Mesh(mesh.devices.reshape(4, 2, 4, 2, 2), EVERY)
    tokens, weights, grads = P(EVERY, None), P(GROUP, None, None), P(GROUP, REPLICA, None)

    return jax.shard_map(
        shards,
        mesh=torus,
        in_specs=(tokens, tokens, tokens, tokens, weights, weights, weights),
        out_specs=(tokens, tokens, grads, grads, grads),
        check_vma=False,
    )
```

```python
import jax
import jax.numpy as jnp
from jax import lax
from jax.experimental import pallas as pl
from jax.experimental.pallas import tpu as pltpu
from jax.sharding import Mesh
from jax.sharding import PartitionSpec as P


F32 = jnp.float32
BF16 = jnp.bfloat16
GROUP = ("zl", "c")
REPLICA = ("x", "zh", "y")
EVERY = ("x", "zh", "y", "zl", "c")
XA, XB, YA, YB, Z = ("x", 1), ("x", 3), ("y", 1), ("y", 3), ("zh", 1)
ORDERS = ((XA, XB, YA, YB, Z), (YA, YB, XA, XB, Z), (XB, XA, YB, YA, Z), (YB, YA, XB, XA, Z))
DOWN_ORDERS = ORDERS[:2] + ((Z, XA, YB, YA, XB), (Z, YA, XB, XA, YB))
CHAINS = (2, 3, 0, 1)
BLOCKS = 32
HALF = BLOCKS // 2
PIECE = 128
LANES = 128
ROW = ((8, LANES), F32)


def moved(array, axis, mask):
    return lax.ppermute(array, axis, [(i, i ^ mask) for i in range(lax.axis_size(axis))])


def block_at(order, pos):
    masks = dict.fromkeys(REPLICA, 0)
    for step, (axis, mask) in enumerate(order):
        if pos >> (4 - step) & 1:
            masks[axis] ^= mask
    x, z, y = (lax.axis_index(axis) ^ masks[axis] for axis in REPLICA)
    return (x * 2 + z) * 4 + y


def group_index():
    return lax.axis_index("zl") * 2 + lax.axis_index("c")


def as_row(column):
    return jnp.broadcast_to(column, (column.shape[0], LANES)).T[:8]


def as_column(row):
    return jnp.broadcast_to(row[0:1, :], (LANES, LANES)).T[:, 0:1]


def nt(a, b):
    return lax.dot_general(a, b, (((1,), (1,)), ((), ())), preferred_element_type=F32)


def nn(a, b):
    return jnp.dot(a, b, preferred_element_type=F32)


def kernel(body, ins, outs, limit, flops, scratch=()):
    vmem = pl.BlockSpec(memory_space=pltpu.VMEM)
    return pl.pallas_call(
        body,
        in_specs=[vmem] * len(ins),
        out_specs=[vmem] * len(outs),
        out_shape=[jax.ShapeDtypeStruct(s, t) for s, t in outs],
        scratch_shapes=list(scratch),
        compiler_params=pltpu.CompilerParams(vmem_limit_bytes=limit << 20),
        cost_estimate=pl.CostEstimate(flops=flops, transcendentals=0, bytes_accessed=1 << 20),
    )(*ins)


def route_body(ids, combine, *outs):
    mine = group_index()
    for m, out in enumerate(outs):
        chosen = ids[...] == (mine ^ m)
        row = jnp.sum(jnp.where(chosen, combine[...], 0.0), axis=0, keepdims=True)
        out[...] = jnp.broadcast_to(row, out.shape)


def combine_body(ids, c0, c1, c2, c3, out):
    mine = group_index()
    total = jnp.zeros(out.shape, F32)
    for m, c in enumerate((c0, c1, c2, c3)):
        total = total + jnp.where(ids[...] == (mine ^ m), c[0:1, :], 0.0)
    out[...] = total


def forward_body(x0, x1, c0, c1, wg, wu, slope, act_out, hid, cht, xt, xs):
    cw = jnp.concatenate([as_column(c0[...]), as_column(c1[...])], axis=0)
    for j, x in enumerate((x0, x1)):
        xs[pl.ds(j * PIECE, PIECE), :] = x[...]
    tile = 256
    for f in range(wg.shape[1] // tile):
        at = pl.ds(f * tile, tile)
        gate = nn(xs[...], wg[:, at])
        up = nn(xs[...], wu[:, at])
        sig = jax.nn.sigmoid(gate)
        act = gate * sig
        slope[:, at] = up * (sig * (1.0 + gate * (1.0 - sig)))
        act_out[:, at] = act
        hidden = act * up
        hid[:, at] = hidden.astype(BF16)
        cht[at, :] = (cw * hidden).T
    for j in range(2):
        xt[:, pl.ds(j * PIECE, PIECE)] = xs[pl.ds(j * PIECE, PIECE), :].T


def forward(x0, x1, cws, wg, wu):
    d, ff = wg.shape
    rows = 2 * PIECE
    outs = [((rows, ff), F32), ((rows, ff), F32), ((rows, ff), BF16), ((ff, rows), F32), ((d, rows), BF16)]
    return kernel(
        forward_body,
        (x0, x1, *cws, wg, wu),
        outs,
        12,
        4 * rows * d * ff,
        scratch=(pltpu.VMEM((rows, d), BF16),),
    )


def down_body(first, chunk, hta, htb, g0, g1, g2, g3, *refs):
    outs, (mixed, gs) = refs[:-2], refs[-2:]
    cols = g2.shape[1] // 2
    for j, g in enumerate((g0, g1)):
        gs[pl.ds(j * PIECE, PIECE), :] = g[:, pl.ds(chunk * 2 * cols, 2 * cols)]
    for j, g in enumerate((g2, g3)):
        gs[pl.ds((2 + j) * PIECE, PIECE), :] = g[...]
    size = hta.shape[0] // BLOCKS
    rows = hta.shape[1]
    for q in range(2):
        out = outs[q % len(outs)]
        base = q * (out.shape[0] // 2) if len(outs) == 1 else 0
        for b in range(HALF):
            start = pl.multiple_of(block_at(DOWN_ORDERS[2 * chunk + q], first + b) * size, 8)
            mixed[q, pl.ds(b * size, size), pl.ds(0, rows)] = hta[pl.ds(start, size), :]
            mixed[q, pl.ds(b * size, size), pl.ds(rows, rows)] = htb[pl.ds(start, size), :]
        part = nn(mixed[q].astype(BF16), gs[:, pl.ds(q * cols, cols)])
        for b in range(HALF):
            block = part[b * size : (b + 1) * size]
            stack = [block[:, k * LANES : (k + 1) * LANES] for k in range(cols // LANES)]
            tall = size * len(stack)
            out[pl.ds(base + b * tall, tall), :] = jnp.concatenate(stack, axis=0).astype(BF16)


def down_half(first, chunk, hts, pieces, joint=False):
    ff, rows = hts[0].shape
    width = pieces[2].shape[1]
    count = 1 if joint else 2
    out = ((2 // count * HALF * ff // BLOCKS * (width // 2 // LANES), LANES), BF16)

    def body(*refs):
        down_body(first, chunk, *refs)

    return kernel(
        body,
        (*hts, *pieces),
        [out] * count,
        12,
        2 * rows * ff * width,
        scratch=(pltpu.VMEM((2, ff // 2, 2 * rows), F32), pltpu.VMEM((2 * rows, width), BF16)),
    )


def hidden_body(pieces, c0, c1, wd, slope, act, hid, gd, ud, comb0, comb1, gs):
    cw = jnp.concatenate([as_column(c0[...]), as_column(c1[...])], axis=0)
    for j, chunks in enumerate(pieces):
        at = 0
        for g in chunks:
            gs[pl.ds(j * PIECE, PIECE), pl.ds(at, g.shape[1])] = g[...]
            at += g.shape[1]
    tile = 256
    total = jnp.zeros((gs.shape[0], 1), F32)
    for f in range(wd.shape[0] // tile):
        at = pl.ds(f * tile, tile)
        back = nt(gs[...], wd[at, :])
        total = total + jnp.sum(hid[:, at].astype(F32) * back, axis=1, keepdims=True)
        back = cw * back
        gd[:, at] = (back * slope[:, at]).astype(BF16)
        ud[:, at] = (back * act[:, at]).astype(BF16)
    comb0[...] = as_row(total[:PIECE])
    comb1[...] = as_row(total[PIECE:])


def hidden_part(pieces, cws, wd, slope, act, hid):
    ff, d = wd.shape
    rows = 2 * PIECE
    counts = [len(chunks) for chunks in pieces]

    def body(*refs):
        first, second = refs[: counts[0]], refs[counts[0] : sum(counts)]
        hidden_body((first, second), *refs[sum(counts) :])

    return kernel(
        body,
        (*pieces[0], *pieces[1], *cws, wd, slope, act, hid),
        [((rows, ff), BF16), ((rows, ff), BF16), ROW, ROW],
        10,
        2 * rows * d * ff,
        scratch=(pltpu.VMEM((rows, d), BF16),),
    )


def gate_body(first, xta, xtb, gda, gdb, uda, udb, *refs):
    outs, mixed = refs[:4], refs[4]
    size = xta.shape[0] // BLOCKS // 2
    rows = xta.shape[1]
    for p in range(4):
        for b in range(HALF):
            start = pl.multiple_of(block_at(ORDERS[p], first + b) * (2 * size) + (p % 2) * size, size)
            mixed[p, pl.ds(b * size, size), pl.ds(0, rows)] = xta[pl.ds(start, size), :]
            mixed[p, pl.ds(b * size, size), pl.ds(rows, rows)] = xtb[pl.ds(start, size), :]
        ga, gb = (gda, gdb) if p < 2 else (uda, udb)
        cols = ga.shape[1]
        tile = 256
        per = tile // LANES
        tall = size * (cols // LANES)
        for n in range(cols // tile):
            at = pl.ds(n * tile, tile)
            part = nn(mixed[p, :, pl.ds(0, rows)], ga[:, at]) + nn(mixed[p, :, pl.ds(rows, rows)], gb[:, at])
            part = part.astype(BF16)
            for b in range(HALF):
                for k in range(per):
                    to = b * tall + (n * per + k) * size
                    outs[p][pl.ds(to, size), :] = part[b * size : (b + 1) * size, k * LANES : (k + 1) * LANES]


def gate_half(first, xts, gds, uds):
    d, rows = xts[0].shape
    ff = gds[0].shape[1]
    out = ((HALF * (d // BLOCKS // 2) * (ff // LANES), LANES), BF16)

    def body(*refs):
        gate_body(first, *refs)

    return kernel(
        body,
        (*xts, *gds, *uds),
        [out] * 4,
        12,
        4 * rows * ff * d,
        scratch=(pltpu.VMEM((4, d // 4, 2 * rows), BF16),),
    )


def rows_body(gda, gdb, uda, udb, wg, wu, r0, r1, r2, r3, gd, ud):
    half = gda.shape[0]
    for scratch, pair in ((gd, (gda, gdb)), (ud, (uda, udb))):
        for j, ref in enumerate(pair):
            scratch[pl.ds(j * half, half), :] = ref[...]
    tile = 512
    for n in range(wg.shape[0] // tile):
        at = pl.ds(n * tile, tile)
        total = (nt(gd[...], wg[at, :]) + nt(ud[...], wu[at, :])).astype(BF16)
        for j, r in enumerate((r0, r1, r2, r3)):
            r[:, at] = total[j * PIECE : (j + 1) * PIECE, :]


def finish_body(*refs):
    bases, (last_a, end2, end3, last_b), (gate, up, down) = refs[:8], refs[8:12], refs[12:]
    first, second = last_a[...].astype(F32), last_b[...].astype(F32)
    tall, low = bases[0].shape[0], bases[4].shape[0]
    recvs = [second[:tall], second[tall : 2 * tall], first[:tall], first[tall:]]
    recvs += [second[2 * tall : 2 * tall + low], second[2 * tall + low :]]
    recvs += [end2[...].astype(F32), end3[...].astype(F32)]
    total = jnp.concatenate([b[...] + r for b, r in zip(bases, recvs)], axis=0)
    half, low = gate.shape[0] // 2, down.shape[0]
    cols = down.shape[1] // 4
    at = 0
    for p in range(4):
        out = gate if p < 2 else up
        for k in range(gate.shape[1] // LANES):
            block = total[at : at + half].astype(BF16)
            out[pl.ds(p % 2 * half, half), pl.ds(k * LANES, LANES)] = block
            at += half
    for p in range(4):
        for k in range(cols // LANES):
            block = total[at : at + low].astype(BF16)
            down[:, pl.ds(p * cols + k * LANES, LANES)] = block
            at += low


def summed(arrays, start, stop, kind=BF16):
    total = 0.0
    for blocks, a in arrays:
        size = a.shape[0] // blocks
        total = total + a[start * size : stop * size].astype(F32)
    return total.astype(kind)


def shards(tokens, cotangent, expert_ids, combine, w_gate, w_up, w_down):
    wg, wu, wd = w_gate[0], w_up[0], w_down[0]
    d, ff = wg.shape
    rows = 4 * PIECE

    tok_far = moved(tokens, "zl", 1)
    tok_near = moved(tokens, "c", 1)
    own = kernel(route_body, (expert_ids.T, combine.T), [ROW] * 4, 2, 1 << 10)
    cws = [own[0]] + [moved(own[m], GROUP, m) for m in (1, 2, 3)]
    cwa, cwb = cws[:2], cws[2:]
    cot_near = moved(cotangent, "c", 1)
    cot_far = [moved(cotangent[:, k * d // 2 : (k + 1) * d // 2], "zl", 1) for k in range(2)]
    tok_both = moved(tok_far, "c", 1)
    cot_both = [moved(cot_far[k], "c", 1) for k in range(2)]

    fa = forward(tokens, tok_near, cwa, wg, wu)
    fb = forward(tok_far, tok_both, cwb, wg, wu)
    hts, xts = (fa[3], fb[3]), (fa[4], fb[4])
    pieces = [(cotangent, cot_near, cot_far[k], cot_both[k]) for k in range(2)]
    down_send = down_half(HALF, 0, hts, pieces[0])
    down_z = down_half(HALF, 1, hts, pieces[1], joint=True)[0]
    ha = hidden_part(((cotangent,), (cot_near,)), cwa, wd, *fa[:3])
    hb = hidden_part((cot_far, cot_both), cwb, wd, *fb[:3])
    gds, uds = (ha[0], hb[0]), (ha[1], hb[1])
    gate_send = gate_half(HALF, xts, gds, uds)
    down_keep = [a for k in range(2) for a in down_half(0, k, hts, pieces[k])]
    gate_keep = gate_half(0, xts, gds, uds)
    grads = kernel(
        rows_body,
        (*gds, *uds, wg, wu),
        [((PIECE, d), BF16)] * 4,
        12,
        4 * rows * d * ff,
        scratch=(pltpu.VMEM((rows, ff), BF16),) * 2,
    )

    down_z = moved(down_z, *Z)
    size = down_z.shape[0] // 2
    down_got = [moved(down_send[p], *ORDERS[p][0]) for p in (0, 1)]
    down_got += [lax.optimization_barrier(a) for a in (down_z[:size], down_z[size:])]
    have = [
        [
            [(HALF, gate_keep[p]), (HALF, moved(gate_send[p], *ORDERS[p][0]))],
            [(HALF, down_keep[p]), (HALF, down_got[p])],
        ]
        for p in range(4)
    ]

    gates, downs = ([have[p][k] for p in range(4)] for k in (0, 1))
    left = {id(h): HALF for h in gates + downs}

    def exchange(held, step):
        sends = [summed(h, left[id(h)] // 2, left[id(h)]) for h in held]
        sent = jnp.concatenate(sends, axis=0)
        got = moved(sent, *step)
        at = 0
        for h, send in zip(held, sends):
            left[id(h)] //= 2
            h.append((left[id(h)], got[at : at + send.shape[0]]))
            at += send.shape[0]
        return got

    for p in CHAINS:
        exchange(have[p][: 2 if p < 2 else 1], ORDERS[p][1])
    for p in (2, 3):
        exchange(downs[p : p + 1], DOWN_ORDERS[p][1])
    for step in (2, 3):
        for p in CHAINS:
            exchange(have[p], ORDERS[p][step])
    last_a = exchange(gates[2:], Z)
    ends = [exchange(downs[p : p + 1], DOWN_ORDERS[p][4]) for p in (2, 3)]
    last_b = exchange(gates[:2] + downs[:2], Z)
    bases = [summed(h[:-1], 0, 1, F32) for h in gates + downs]
    gate_grad, up_grad, down_grad = kernel(
        finish_body,
        (*bases, last_a, *ends, last_b),
        [((d // BLOCKS, ff), BF16), ((d // BLOCKS, ff), BF16), ((ff // BLOCKS, d), BF16)],
        4,
        1 << 20,
    )

    near = moved(grads[1], "c", 1)
    far = (grads[2].astype(F32) + moved(grads[3], "c", 1).astype(F32)).astype(BF16)
    far = moved(far, "zl", 1)
    input_grad = (grads[0].astype(F32) + near.astype(F32) + far.astype(F32)).astype(BF16)

    comb = [ha[2], ha[3], hb[2], hb[3]]
    given = [comb[0]] + [moved(comb[m], GROUP, m) for m in (1, 2, 3)]
    combine_grad = kernel(combine_body, (expert_ids.T, *given), [((2, PIECE), F32)], 2, 1 << 10)[0].T
    return (input_grad, combine_grad, gate_grad[None], up_grad[None], down_grad[None])


def solution(mesh):
    torus = Mesh(mesh.devices.reshape(4, 2, 4, 2, 2), EVERY)
    tokens, weights, grads = P(EVERY, None), P(GROUP, None, None), P(GROUP, REPLICA, None)

    return jax.shard_map(
        shards,
        mesh=torus,
        in_specs=(tokens, tokens, tokens, tokens, weights, weights, weights),
        out_specs=(tokens, tokens, grads, grads, grads),
        check_vma=False,
    )
```

```python
import jax
import jax.numpy as jnp
from jax import lax
from jax.experimental import pallas as pl
from jax.experimental.pallas import tpu as pltpu
from jax.sharding import Mesh
from jax.sharding import PartitionSpec as P


F32 = jnp.float32
BF16 = jnp.bfloat16
GROUP = ("zl", "c")
REPLICA = ("x", "zh", "y")
EVERY = ("x", "zh", "y", "zl", "c")
XA, XB, YA, YB, Z = ("x", 1), ("x", 3), ("y", 1), ("y", 3), ("zh", 1)
ORDERS = ((XA, XB, YA, YB, Z), (YA, YB, XA, XB, Z), (XB, XA, YB, YA, Z), (YB, YA, XB, XA, Z))
DOWN_ORDERS = ORDERS[:2] + ((Z, XB, XA, YB, YA), (Z, YB, YA, XB, XA))
CHAINS = (2, 3, 0, 1)
BLOCKS = 32
HALF = BLOCKS // 2
PIECE = 128
LANES = 128
ROW = ((8, LANES), F32)


def moved(array, axis, mask):
    return lax.ppermute(array, axis, [(i, i ^ mask) for i in range(lax.axis_size(axis))])


def block_at(order, pos):
    masks = dict.fromkeys(REPLICA, 0)
    for step, (axis, mask) in enumerate(order):
        if pos >> (4 - step) & 1:
            masks[axis] ^= mask
    x, z, y = (lax.axis_index(axis) ^ masks[axis] for axis in REPLICA)
    return (x * 2 + z) * 4 + y


def group_index():
    return lax.axis_index("zl") * 2 + lax.axis_index("c")


def as_row(column):
    return jnp.broadcast_to(column, (column.shape[0], LANES)).T[:8]


def as_column(row):
    return jnp.broadcast_to(row[0:1, :], (LANES, LANES)).T[:, 0:1]


def nt(a, b):
    return lax.dot_general(a, b, (((1,), (1,)), ((), ())), preferred_element_type=F32)


def nn(a, b):
    return jnp.dot(a, b, preferred_element_type=F32)


def kernel(body, ins, outs, limit, flops, scratch=()):
    vmem = pl.BlockSpec(memory_space=pltpu.VMEM)
    return pl.pallas_call(
        body,
        in_specs=[vmem] * len(ins),
        out_specs=[vmem] * len(outs),
        out_shape=[jax.ShapeDtypeStruct(s, t) for s, t in outs],
        scratch_shapes=list(scratch),
        compiler_params=pltpu.CompilerParams(vmem_limit_bytes=limit << 20),
        cost_estimate=pl.CostEstimate(flops=flops, transcendentals=0, bytes_accessed=1 << 20),
    )(*ins)


def route_body(ids, combine, *outs):
    mine = group_index()
    for m, out in enumerate(outs):
        chosen = ids[...] == (mine ^ m)
        row = jnp.sum(jnp.where(chosen, combine[...], 0.0), axis=0, keepdims=True)
        out[...] = jnp.broadcast_to(row, out.shape)


def combine_body(ids, c0, c1, c2, c3, out):
    mine = group_index()
    total = jnp.zeros(out.shape, F32)
    for m, c in enumerate((c0, c1, c2, c3)):
        total = total + jnp.where(ids[...] == (mine ^ m), c[0:1, :], 0.0)
    out[...] = total


def forward_body(x0, x1, c0, c1, wg, wu, slope, act_out, hid, cht, xt, xs):
    cw = jnp.concatenate([as_column(c0[...]), as_column(c1[...])], axis=0)
    for j, x in enumerate((x0, x1)):
        xs[pl.ds(j * PIECE, PIECE), :] = x[...]
    tile = 256
    for f in range(wg.shape[1] // tile):
        at = pl.ds(f * tile, tile)
        gate = nn(xs[...], wg[:, at])
        up = nn(xs[...], wu[:, at])
        sig = jax.nn.sigmoid(gate)
        act = gate * sig
        slope[:, at] = up * (sig * (1.0 + gate * (1.0 - sig)))
        act_out[:, at] = act
        hidden = act * up
        hid[:, at] = hidden.astype(BF16)
        cht[at, :] = (cw * hidden).T
    for j in range(2):
        xt[:, pl.ds(j * PIECE, PIECE)] = xs[pl.ds(j * PIECE, PIECE), :].T


def forward(x0, x1, cws, wg, wu):
    d, ff = wg.shape
    rows = 2 * PIECE
    outs = [((rows, ff), F32), ((rows, ff), F32), ((rows, ff), BF16), ((ff, rows), F32), ((d, rows), BF16)]
    return kernel(
        forward_body, (x0, x1, *cws, wg, wu), outs, 12, 4 * rows * d * ff, scratch=(pltpu.VMEM((rows, d), BF16),)
    )


def down_body(first, chunk, hta, htb, g0, g1, g2, g3, *refs):
    outs, (mixed, gs) = refs[:-2], refs[-2:]
    cols = g2.shape[1] // 2
    for j, g in enumerate((g0, g1)):
        gs[pl.ds(j * PIECE, PIECE), :] = g[:, pl.ds(chunk * 2 * cols, 2 * cols)]
    for j, g in enumerate((g2, g3)):
        gs[pl.ds((2 + j) * PIECE, PIECE), :] = g[...]
    size = hta.shape[0] // BLOCKS
    rows = hta.shape[1]
    for q in range(2):
        out = outs[q % len(outs)]
        base = q * (out.shape[0] // 2) if len(outs) == 1 else 0
        for b in range(HALF):
            start = pl.multiple_of(block_at(DOWN_ORDERS[2 * chunk + q], first + b) * size, 8)
            mixed[q, pl.ds(b * size, size), pl.ds(0, rows)] = hta[pl.ds(start, size), :]
            mixed[q, pl.ds(b * size, size), pl.ds(rows, rows)] = htb[pl.ds(start, size), :]
        part = nn(mixed[q].astype(BF16), gs[:, pl.ds(q * cols, cols)])
        for b in range(HALF):
            block = part[b * size : (b + 1) * size]
            stack = [block[:, k * LANES : (k + 1) * LANES] for k in range(cols // LANES)]
            tall = size * len(stack)
            out[pl.ds(base + b * tall, tall), :] = jnp.concatenate(stack, axis=0).astype(BF16)


def down_half(first, chunk, hts, pieces, joint=False):
    ff, rows = hts[0].shape
    width = pieces[2].shape[1]
    count = 1 if joint else 2
    out = ((2 // count * HALF * ff // BLOCKS * (width // 2 // LANES), LANES), BF16)

    def body(*refs):
        down_body(first, chunk, *refs)

    return kernel(
        body,
        (*hts, *pieces),
        [out] * count,
        12,
        2 * rows * ff * width,
        scratch=(pltpu.VMEM((2, ff // 2, 2 * rows), F32), pltpu.VMEM((2 * rows, width), BF16)),
    )


def hidden_body(pieces, c0, c1, wd, slope, act, hid, gd, ud, comb0, comb1, gs):
    cw = jnp.concatenate([as_column(c0[...]), as_column(c1[...])], axis=0)
    for j, chunks in enumerate(pieces):
        at = 0
        for g in chunks:
            gs[pl.ds(j * PIECE, PIECE), pl.ds(at, g.shape[1])] = g[...]
            at += g.shape[1]
    tile = 256
    total = jnp.zeros((gs.shape[0], 1), F32)
    for f in range(wd.shape[0] // tile):
        at = pl.ds(f * tile, tile)
        back = nt(gs[...], wd[at, :])
        total = total + jnp.sum(hid[:, at].astype(F32) * back, axis=1, keepdims=True)
        back = cw * back
        gd[:, at] = (back * slope[:, at]).astype(BF16)
        ud[:, at] = (back * act[:, at]).astype(BF16)
    comb0[...] = as_row(total[:PIECE])
    comb1[...] = as_row(total[PIECE:])


def hidden_part(pieces, cws, wd, slope, act, hid):
    ff, d = wd.shape
    rows = 2 * PIECE
    counts = [len(chunks) for chunks in pieces]

    def body(*refs):
        first, second = refs[: counts[0]], refs[counts[0] : sum(counts)]
        hidden_body((first, second), *refs[sum(counts) :])

    return kernel(
        body,
        (*pieces[0], *pieces[1], *cws, wd, slope, act, hid),
        [((rows, ff), BF16), ((rows, ff), BF16), ROW, ROW],
        10,
        2 * rows * d * ff,
        scratch=(pltpu.VMEM((rows, d), BF16),),
    )


TILE = 256
EARLY = ((2, 0, 3), (3, 0, 3))
LATER = ((0, 0, 2), (1, 0, 2), (0, 2, 3), (1, 2, 3))


def gate_body(first, specs, xta, xtb, gda, gdb, uda, udb, *refs):
    outs, mixed = refs[:-1], refs[-1]
    size = xta.shape[0] // BLOCKS // 2
    rows = xta.shape[1]
    chains = []
    for (p, low, high), out in zip(specs, outs):
        if p not in chains:
            chains.append(p)
            at = chains.index(p)
            for b in range(HALF):
                start = pl.multiple_of(block_at(ORDERS[p], first + b) * (2 * size) + (p % 2) * size, size)
                mixed[at, pl.ds(b * size, size), pl.ds(0, rows)] = xta[pl.ds(start, size), :]
                mixed[at, pl.ds(b * size, size), pl.ds(rows, rows)] = xtb[pl.ds(start, size), :]
        q = chains.index(p)
        ga, gb = (gda, gdb) if p < 2 else (uda, udb)
        per = TILE // LANES
        tall = size * per * (high - low)
        for n in range(low, high):
            at = pl.ds(n * TILE, TILE)
            part = nn(mixed[q, :, pl.ds(0, rows)], ga[:, at]) + nn(mixed[q, :, pl.ds(rows, rows)], gb[:, at])
            part = part.astype(BF16)
            for b in range(HALF):
                for k in range(per):
                    to = b * tall + ((n - low) * per + k) * size
                    out[pl.ds(to, size), :] = part[b * size : (b + 1) * size, k * LANES : (k + 1) * LANES]


def gate_half(first, specs, xts, gds, uds):
    d, rows = xts[0].shape
    tiles = [high - low for _, low, high in specs]
    outs = [((HALF * (d // BLOCKS // 2) * t * (TILE // LANES), LANES), BF16) for t in tiles]

    def body(*refs):
        gate_body(first, specs, *refs)

    return kernel(
        body,
        (*xts, *gds, *uds),
        outs,
        12,
        d * rows * TILE * sum(tiles),
        scratch=(pltpu.VMEM((len({p for p, _, _ in specs}), d // 4, 2 * rows), BF16),),
    )


def rows_body(gda, gdb, uda, udb, wg, wu, r0, r1, r2, r3, gd, ud):
    half = gda.shape[0]
    for scratch, pair in ((gd, (gda, gdb)), (ud, (uda, udb))):
        for j, ref in enumerate(pair):
            scratch[pl.ds(j * half, half), :] = ref[...]
    tile = 512
    for n in range(wg.shape[0] // tile):
        at = pl.ds(n * tile, tile)
        total = (nt(gd[...], wg[at, :]) + nt(ud[...], wu[at, :])).astype(BF16)
        for j, r in enumerate((r0, r1, r2, r3)):
            r[:, at] = total[j * PIECE : (j + 1) * PIECE, :]


def finish_body(*refs):
    bases, (last_a, last_b), (gate, up, down) = refs[:-5], refs[-5:-3], refs[-3:]
    recv = {0: (last_b[...].astype(F32), 0), 2: (last_a[...].astype(F32), 0)}
    half, low = gate.shape[0] // 2, down.shape[0]
    cols = down.shape[1] // 4
    done = []
    for n, base in enumerate(bases):
        rows = base.shape[0]
        p = (EARLY + LATER)[n][0] if n < 6 else n - 6
        if n < 6 or p < 2:
            array, at = recv[p // 2 * 2]
            done.append(base[...] + array[at : at + rows])
            recv[p // 2 * 2] = (array, at + rows)
        else:
            done.append(base[...])
    for (p, first, _), total in zip(EARLY + LATER, done):
        out = gate if p < 2 else up
        for k in range(total.shape[0] // half):
            to = first * TILE + k * LANES
            out[pl.ds(p % 2 * half, half), pl.ds(to, LANES)] = total[k * half : (k + 1) * half].astype(BF16)
    for p, total in enumerate(done[6:]):
        for k in range(cols // LANES):
            down[:, pl.ds(p * cols + k * LANES, LANES)] = total[k * low : (k + 1) * low].astype(BF16)


def summed(arrays, start, stop, kind=BF16):
    total = 0.0
    for blocks, a in arrays:
        size = a.shape[0] // blocks
        total = total + a[start * size : stop * size].astype(F32)
    return total.astype(kind)


def shards(tokens, cotangent, expert_ids, combine, w_gate, w_up, w_down):
    wg, wu, wd = w_gate[0], w_up[0], w_down[0]
    d, ff = wg.shape
    rows = 4 * PIECE

    tok_far = moved(tokens, "zl", 1)
    tok_near = moved(tokens, "c", 1)
    own = kernel(route_body, (expert_ids.T, combine.T), [ROW] * 4, 2, 1 << 10)
    cws = [own[0]] + [moved(own[m], GROUP, m) for m in (1, 2, 3)]
    cwa, cwb = cws[:2], cws[2:]
    cot_near = moved(cotangent, "c", 1)
    cot_far = [moved(cotangent[:, k * d // 2 : (k + 1) * d // 2], "zl", 1) for k in range(2)]
    tok_both = moved(tok_far, "c", 1)
    cot_both = [moved(cot_far[k], "c", 1) for k in range(2)]

    fa = forward(tokens, tok_near, cwa, wg, wu)
    fb = forward(tok_far, tok_both, cwb, wg, wu)
    hts, xts = (fa[3], fb[3]), (fa[4], fb[4])
    pieces = [(cotangent, cot_near, cot_far[k], cot_both[k]) for k in range(2)]
    down_send = down_half(HALF, 0, hts, pieces[0])
    down_z = down_half(HALF, 1, hts, pieces[1], joint=True)[0]
    ha = hidden_part(((cotangent,), (cot_near,)), cwa, wd, *fa[:3])
    hb = hidden_part((cot_far, cot_both), cwb, wd, *fb[:3])
    gds, uds = (ha[0], hb[0]), (ha[1], hb[1])
    gate_send = list(gate_half(HALF, EARLY, xts, gds, uds))
    gate_send += gate_half(HALF, LATER, xts, gds, uds)
    down_keep = [a for k in range(2) for a in down_half(0, k, hts, pieces[k])]
    gate_keep = gate_half(0, EARLY + LATER, xts, gds, uds)
    grads = kernel(
        rows_body,
        (*gds, *uds, wg, wu),
        [((PIECE, d), BF16)] * 4,
        12,
        4 * rows * d * ff,
        scratch=(pltpu.VMEM((rows, ff), BF16),) * 2,
    )

    down_z = moved(down_z, *Z)
    size = down_z.shape[0] // 2
    down_got = [moved(down_send[p], *ORDERS[p][0]) for p in (0, 1)]
    down_got += [lax.optimization_barrier(a) for a in (down_z[:size], down_z[size:])]
    gates, downs = [], [[(HALF, down_keep[p]), (HALF, down_got[p])] for p in range(4)]
    for spec, keep, send in zip(EARLY + LATER, gate_keep, gate_send):
        gates.append([(HALF, keep), (HALF, moved(send, *ORDERS[spec[0]][0]))])
    have = [[g for g, spec in zip(gates, EARLY + LATER) if spec[0] == p] + [downs[p]] for p in range(4)]
    left = {id(h): HALF for h in gates + downs}

    def exchange(held, step):
        sends = [summed(h, left[id(h)] // 2, left[id(h)]) for h in held]
        sent = jnp.concatenate(sends, axis=0)
        got = moved(sent, *step)
        at = 0
        for h, send in zip(held, sends):
            left[id(h)] //= 2
            h.append((left[id(h)], got[at : at + send.shape[0]]))
            at += send.shape[0]
        return got

    for p in (0, 1):
        exchange(have[p][:1], ORDERS[p][1])
    for p in (2, 3):
        exchange(have[p][:1], ORDERS[p][1])
    for p in (2, 3):
        exchange(downs[p : p + 1], DOWN_ORDERS[p][1])
    for p in (0, 1):
        exchange(have[p][1:], ORDERS[p][1])
    for p in (2, 3):
        exchange(downs[p : p + 1], DOWN_ORDERS[p][2])
    for step in (2, 3):
        for p in CHAINS:
            exchange(have[p], ORDERS[p][step])
    last_a = exchange(gates[:2], Z)
    last_b = exchange(gates[2:] + downs[:2], Z)
    bases = [summed(h[:-1], 0, 1, F32) for h in gates + downs[:2]] + [summed(h, 0, 1, F32) for h in downs[2:]]
    gate_grad, up_grad, down_grad = kernel(
        finish_body,
        (*bases, last_a, last_b),
        [((d // BLOCKS, ff), BF16), ((d // BLOCKS, ff), BF16), ((ff // BLOCKS, d), BF16)],
        4,
        1 << 20,
    )

    near = moved(grads[1], "c", 1)
    far = (grads[2].astype(F32) + moved(grads[3], "c", 1).astype(F32)).astype(BF16)
    far = moved(far, "zl", 1)
    input_grad = (grads[0].astype(F32) + near.astype(F32) + far.astype(F32)).astype(BF16)

    comb = [ha[2], ha[3], hb[2], hb[3]]
    given = [comb[0]] + [moved(comb[m], GROUP, m) for m in (1, 2, 3)]
    combine_grad = kernel(combine_body, (expert_ids.T, *given), [((2, PIECE), F32)], 2, 1 << 10)[0].T
    return (input_grad, combine_grad, gate_grad[None], up_grad[None], down_grad[None])


def solution(mesh):
    torus = Mesh(mesh.devices.reshape(4, 2, 4, 2, 2), EVERY)
    tokens, weights, grads = P(EVERY, None), P(GROUP, None, None), P(GROUP, REPLICA, None)

    return jax.shard_map(
        shards,
        mesh=torus,
        in_specs=(tokens, tokens, tokens, tokens, weights, weights, weights),
        out_specs=(tokens, tokens, grads, grads, grads),
        check_vma=False,
    )
```

```python
import jax
import jax.numpy as jnp
from jax import lax
from jax.experimental import pallas as pl
from jax.experimental.pallas import tpu as pltpu
from jax.sharding import Mesh
from jax.sharding import PartitionSpec as P


F32 = jnp.float32
BF16 = jnp.bfloat16
GROUP = ("zl", "c")
REPLICA = ("x", "zh", "y")
EVERY = ("x", "zh", "y", "zl", "c")
XA, XB, YA, YB, Z = ("x", 1), ("x", 3), ("y", 1), ("y", 3), ("zh", 1)
ORDERS = ((XA, XB, YA, YB, Z), (YA, YB, XA, XB, Z), (XB, XA, YB, YA, Z), (YB, YA, XB, XA, Z))
DOWN_ORDERS = ORDERS[:2] + ((Z, XB, XA, YB, YA), (Z, YB, YA, XB, XA))
CHAINS = (2, 3, 0, 1)
BLOCKS = 32
HALF = BLOCKS // 2
PIECE = 128
LANES = 128
ROW = ((8, LANES), F32)


def moved(array, axis, mask):
    return lax.ppermute(array, axis, [(i, i ^ mask) for i in range(lax.axis_size(axis))])


def block_at(order, pos):
    masks = dict.fromkeys(REPLICA, 0)
    for step, (axis, mask) in enumerate(order):
        if pos >> (4 - step) & 1:
            masks[axis] ^= mask
    x, z, y = (lax.axis_index(axis) ^ masks[axis] for axis in REPLICA)
    return (x * 2 + z) * 4 + y


def group_index():
    return lax.axis_index("zl") * 2 + lax.axis_index("c")


def as_row(column):
    return jnp.broadcast_to(column, (column.shape[0], LANES)).T[:8]


def as_column(row):
    return jnp.broadcast_to(row[0:1, :], (LANES, LANES)).T[:, 0:1]


def nt(a, b):
    return lax.dot_general(a, b, (((1,), (1,)), ((), ())), preferred_element_type=F32)


def nn(a, b):
    return jnp.dot(a, b, preferred_element_type=F32)


def kernel(body, ins, outs, limit, flops, scratch=()):
    vmem = pl.BlockSpec(memory_space=pltpu.VMEM)
    return pl.pallas_call(
        body,
        in_specs=[vmem] * len(ins),
        out_specs=[vmem] * len(outs),
        out_shape=[jax.ShapeDtypeStruct(s, t) for s, t in outs],
        scratch_shapes=list(scratch),
        compiler_params=pltpu.CompilerParams(vmem_limit_bytes=limit << 20),
        cost_estimate=pl.CostEstimate(flops=flops, transcendentals=0, bytes_accessed=1 << 20),
    )(*ins)


def route_body(ids, combine, *outs):
    mine = group_index()
    for m, out in enumerate(outs):
        chosen = ids[...] == (mine ^ m)
        row = jnp.sum(jnp.where(chosen, combine[...], 0.0), axis=0, keepdims=True)
        out[...] = jnp.broadcast_to(row, out.shape)


def forward_body(x0, x1, c0, c1, wg, wu, slope, act_out, hid, cht, xt, xs):
    cw = jnp.concatenate([as_column(c0[...]), as_column(c1[...])], axis=0)
    for j, x in enumerate((x0, x1)):
        xs[pl.ds(j * PIECE, PIECE), :] = x[...]
    tile = 256
    for f in range(wg.shape[1] // tile):
        at = pl.ds(f * tile, tile)
        gate = nn(xs[...], wg[:, at])
        up = nn(xs[...], wu[:, at])
        sig = jax.nn.sigmoid(gate)
        act = gate * sig
        slope[:, at] = up * (sig * (1.0 + gate * (1.0 - sig)))
        act_out[:, at] = act
        hidden = act * up
        hid[:, at] = hidden.astype(BF16)
        cht[at, :] = (cw * hidden).T
    for j in range(2):
        xt[:, pl.ds(j * PIECE, PIECE)] = xs[pl.ds(j * PIECE, PIECE), :].T


def forward(x0, x1, cws, wg, wu):
    d, ff = wg.shape
    rows = 2 * PIECE
    outs = [((rows, ff), F32), ((rows, ff), F32), ((rows, ff), BF16), ((ff, rows), F32), ((d, rows), BF16)]
    return kernel(
        forward_body, (x0, x1, *cws, wg, wu), outs, 12, 4 * rows * d * ff, scratch=(pltpu.VMEM((rows, d), BF16),)
    )


def down_body(first, chunk, hta, htb, g0, g1, g2, g3, *refs):
    outs, (mixed, gs) = refs[:-2], refs[-2:]
    cols = g2.shape[1] // 2
    for j, g in enumerate((g0, g1)):
        gs[pl.ds(j * PIECE, PIECE), :] = g[:, pl.ds(chunk * 2 * cols, 2 * cols)]
    for j, g in enumerate((g2, g3)):
        gs[pl.ds((2 + j) * PIECE, PIECE), :] = g[...]
    size = hta.shape[0] // BLOCKS
    rows = hta.shape[1]
    for q in range(2):
        out = outs[q % len(outs)]
        base = q * (out.shape[0] // 2) if len(outs) == 1 else 0
        for b in range(HALF):
            start = pl.multiple_of(block_at(DOWN_ORDERS[2 * chunk + q], first + b) * size, 8)
            mixed[q, pl.ds(b * size, size), pl.ds(0, rows)] = hta[pl.ds(start, size), :]
            mixed[q, pl.ds(b * size, size), pl.ds(rows, rows)] = htb[pl.ds(start, size), :]
        part = nn(mixed[q].astype(BF16), gs[:, pl.ds(q * cols, cols)])
        for b in range(HALF):
            block = part[b * size : (b + 1) * size]
            stack = [block[:, k * LANES : (k + 1) * LANES] for k in range(cols // LANES)]
            tall = size * len(stack)
            out[pl.ds(base + b * tall, tall), :] = jnp.concatenate(stack, axis=0).astype(BF16)


def down_half(first, chunk, hts, pieces, joint=False):
    ff, rows = hts[0].shape
    width = pieces[2].shape[1]
    count = 1 if joint else 2
    out = ((2 // count * HALF * ff // BLOCKS * (width // 2 // LANES), LANES), BF16)

    def body(*refs):
        down_body(first, chunk, *refs)

    return kernel(
        body,
        (*hts, *pieces),
        [out] * count,
        12,
        2 * rows * ff * width,
        scratch=(pltpu.VMEM((2, ff // 2, 2 * rows), F32), pltpu.VMEM((2 * rows, width), BF16)),
    )


def hidden_body(pieces, c0, c1, wd, slope, act, hid, gd, ud, comb0, comb1, gs):
    cw = jnp.concatenate([as_column(c0[...]), as_column(c1[...])], axis=0)
    for j, chunks in enumerate(pieces):
        at = 0
        for g in chunks:
            gs[pl.ds(j * PIECE, PIECE), pl.ds(at, g.shape[1])] = g[...]
            at += g.shape[1]
    tile = 256
    total = jnp.zeros((gs.shape[0], 1), F32)
    for f in range(wd.shape[0] // tile):
        at = pl.ds(f * tile, tile)
        back = nt(gs[...], wd[at, :])
        total = total + jnp.sum(hid[:, at].astype(F32) * back, axis=1, keepdims=True)
        back = cw * back
        gd[:, at] = (back * slope[:, at]).astype(BF16)
        ud[:, at] = (back * act[:, at]).astype(BF16)
    comb0[...] = as_row(total[:PIECE])
    comb1[...] = as_row(total[PIECE:])


def hidden_part(pieces, cws, wd, slope, act, hid):
    ff, d = wd.shape
    rows = 2 * PIECE
    counts = [len(chunks) for chunks in pieces]

    def body(*refs):
        first, second = refs[: counts[0]], refs[counts[0] : sum(counts)]
        hidden_body((first, second), *refs[sum(counts) :])

    return kernel(
        body,
        (*pieces[0], *pieces[1], *cws, wd, slope, act, hid),
        [((rows, ff), BF16), ((rows, ff), BF16), ROW, ROW],
        10,
        2 * rows * d * ff,
        scratch=(pltpu.VMEM((rows, d), BF16),),
    )


TILE = 256
EARLY = ((2, 0, 3), (3, 0, 3))
LATER = ((0, 0, 3), (1, 0, 3))
EXTRA = 128


def gate_body(first, specs, xta, xtb, gda, gdb, uda, udb, *refs):
    outs, mixed = refs[:-1], refs[-1]
    size = xta.shape[0] // BLOCKS // 2
    rows = xta.shape[1]
    chains = []
    for (p, low, high), out in zip(specs, outs):
        if p not in chains:
            chains.append(p)
            at = chains.index(p)
            for b in range(HALF):
                start = pl.multiple_of(block_at(ORDERS[p], first + b) * (2 * size) + (p % 2) * size, size)
                mixed[at, pl.ds(b * size, size), pl.ds(0, rows)] = xta[pl.ds(start, size), :]
                mixed[at, pl.ds(b * size, size), pl.ds(rows, rows)] = xtb[pl.ds(start, size), :]
        q = chains.index(p)
        ga, gb = (gda, gdb) if p < 2 else (uda, udb)
        per = TILE // LANES
        tall = size * per * (high - low)
        for n in range(low, high):
            at = pl.ds(n * TILE, TILE)
            part = nn(mixed[q, :, pl.ds(0, rows)], ga[:, at]) + nn(mixed[q, :, pl.ds(rows, rows)], gb[:, at])
            part = part.astype(BF16)
            for b in range(HALF):
                for k in range(per):
                    to = b * tall + ((n - low) * per + k) * size
                    out[pl.ds(to, size), :] = part[b * size : (b + 1) * size, k * LANES : (k + 1) * LANES]


def gate_half(first, specs, xts, gds, uds):
    d, rows = xts[0].shape
    tiles = [high - low for _, low, high in specs]
    outs = [((HALF * (d // BLOCKS // 2) * t * (TILE // LANES), LANES), BF16) for t in tiles]

    def body(*refs):
        gate_body(first, specs, *refs)

    return kernel(
        body,
        (*xts, *gds, *uds),
        outs,
        12,
        d * rows * TILE * sum(tiles),
        scratch=(pltpu.VMEM((len({p for p, _, _ in specs}), d // 4, 2 * rows), BF16),),
    )


def rows_body(gda, gdb, uda, udb, wg, wu, *refs):
    combs, (own, side, across, gd, ud) = refs[:4], refs[4:]
    half = gda.shape[0]
    for scratch, pair in ((gd, (gda, gdb)), (ud, (uda, udb))):
        for j, ref in enumerate(pair):
            scratch[pl.ds(j * half, half), :] = ref[...]
    places = ((own, 0), (side, 0), (across, 0), (side, PIECE))
    tile = 512
    for n in range(wg.shape[0] // tile):
        at = pl.ds(n * tile, tile)
        total = (nt(gd[...], wg[at, :]) + nt(ud[...], wu[at, :])).astype(BF16)
        for j, (out, row) in enumerate(places):
            out[pl.ds(row, PIECE), at] = total[j * PIECE : (j + 1) * PIECE, :]
    mine = lax.broadcasted_iota(jnp.int32, (PIECE, EXTRA), 1) == group_index()
    for comb, (out, row) in zip(combs, places):
        value = jnp.where(mine, as_column(comb[...]), 0.0)
        out[pl.ds(row, PIECE), pl.ds(wg.shape[0], EXTRA)] = value.astype(BF16)


def tokens_body(ids, own, side, across, grad, combine):
    total = own[...].astype(F32) + side[pl.ds(0, PIECE), :].astype(F32) + across[...].astype(F32)
    d = grad.shape[1]
    grad[...] = total[:, :d].astype(BF16)
    lanes = total[:, d:].T
    picked = jnp.zeros(combine.shape, F32)
    for e in range(4):
        picked = picked + jnp.where(ids[...] == e, lanes[e : e + 1, :], 0.0)
    combine[...] = picked


def finish_body(*refs):
    bases, (last_a, last_b), (gate, up, down) = refs[:-5], refs[-5:-3], refs[-3:]
    recv = {0: (last_b[...].astype(F32), 0), 2: (last_a[...].astype(F32), 0)}
    half, low = gate.shape[0] // 2, down.shape[0]
    cols = down.shape[1] // 4
    done = []
    for n, base in enumerate(bases):
        rows = base.shape[0]
        p = (EARLY + LATER)[n][0] if n < 4 else n - 4
        if n < 4 or p < 2:
            array, at = recv[p // 2 * 2]
            done.append(base[...] + array[at : at + rows])
            recv[p // 2 * 2] = (array, at + rows)
        else:
            done.append(base[...])
    for (p, first, _), total in zip(EARLY + LATER, done):
        out = gate if p < 2 else up
        for k in range(total.shape[0] // half):
            to = first * TILE + k * LANES
            out[pl.ds(p % 2 * half, half), pl.ds(to, LANES)] = total[k * half : (k + 1) * half].astype(BF16)
    for p, total in enumerate(done[4:]):
        for k in range(cols // LANES):
            down[:, pl.ds(p * cols + k * LANES, LANES)] = total[k * low : (k + 1) * low].astype(BF16)


def summed(arrays, start, stop, kind=BF16):
    total = 0.0
    for blocks, a in arrays:
        size = a.shape[0] // blocks
        total = total + a[start * size : stop * size].astype(F32)
    return total.astype(kind)


def shards(tokens, cotangent, expert_ids, combine, w_gate, w_up, w_down):
    wg, wu, wd = w_gate[0], w_up[0], w_down[0]
    d, ff = wg.shape
    rows = 4 * PIECE

    tok_far = moved(tokens, "zl", 1)
    tok_near = moved(tokens, "c", 1)
    own = kernel(route_body, (expert_ids.T, combine.T), [ROW] * 4, 2, 1 << 10)
    cws = [own[0]] + [moved(own[m], GROUP, m) for m in (1, 2, 3)]
    cwa, cwb = cws[:2], cws[2:]
    cot_near = moved(cotangent, "c", 1)
    cot_far = [moved(cotangent[:, k * d // 2 : (k + 1) * d // 2], "zl", 1) for k in range(2)]
    tok_both = moved(tok_far, "c", 1)
    cot_both = [moved(cot_far[k], "c", 1) for k in range(2)]

    fa = forward(tokens, tok_near, cwa, wg, wu)
    fb = forward(tok_far, tok_both, cwb, wg, wu)
    hts, xts = (fa[3], fb[3]), (fa[4], fb[4])
    pieces = [(cotangent, cot_near, cot_far[k], cot_both[k]) for k in range(2)]
    down_send = down_half(HALF, 0, hts, pieces[0])
    down_z = down_half(HALF, 1, hts, pieces[1], joint=True)[0]
    ha = hidden_part(((cotangent,), (cot_near,)), cwa, wd, *fa[:3])
    hb = hidden_part((cot_far, cot_both), cwb, wd, *fb[:3])
    gds, uds = (ha[0], hb[0]), (ha[1], hb[1])
    gate_send = list(gate_half(HALF, EARLY, xts, gds, uds))
    gate_send += gate_half(HALF, LATER, xts, gds, uds)
    down_keep = [a for k in range(2) for a in down_half(0, k, hts, pieces[k])]
    gate_keep = gate_half(0, EARLY + LATER, xts, gds, uds)
    own_rows, side_rows, far_rows = kernel(
        rows_body,
        (*gds, *uds, wg, wu, ha[2], ha[3], hb[2], hb[3]),
        [((n * PIECE, d + EXTRA), BF16) for n in (1, 2, 1)],
        12,
        4 * rows * d * ff,
        scratch=(pltpu.VMEM((rows, ff), BF16),) * 2,
    )

    down_z = moved(down_z, *Z)
    size = down_z.shape[0] // 2
    down_got = [moved(down_send[p], *ORDERS[p][0]) for p in (0, 1)]
    down_got += [lax.optimization_barrier(a) for a in (down_z[:size], down_z[size:])]
    gates, downs = [], [[(HALF, down_keep[p]), (HALF, down_got[p])] for p in range(4)]
    for spec, keep, send in zip(EARLY + LATER, gate_keep, gate_send):
        gates.append([(HALF, keep), (HALF, moved(send, *ORDERS[spec[0]][0]))])
    have = [[g for g, spec in zip(gates, EARLY + LATER) if spec[0] == p] + [downs[p]] for p in range(4)]
    left = {id(h): HALF for h in gates + downs}

    def exchange(held, step):
        sends = [summed(h, left[id(h)] // 2, left[id(h)]) for h in held]
        sent = jnp.concatenate(sends, axis=0)
        got = moved(sent, *step)
        at = 0
        for h, send in zip(held, sends):
            left[id(h)] //= 2
            h.append((left[id(h)], got[at : at + send.shape[0]]))
            at += send.shape[0]
        return got

    for p in (2, 3):
        exchange(have[p][:1], ORDERS[p][1])
    for p in (2, 3):
        exchange(downs[p : p + 1], DOWN_ORDERS[p][1])
    for p in (0, 1):
        exchange(have[p], ORDERS[p][1])
    for p in (2, 3):
        exchange(downs[p : p + 1], DOWN_ORDERS[p][2])
    for step in (2, 3):
        for p in CHAINS:
            exchange(have[p], ORDERS[p][step])
    last_a = exchange(gates[:2], Z)
    last_b = exchange(gates[2:] + downs[:2], Z)
    bases = [summed(h[:-1], 0, 1, F32) for h in gates + downs[:2]] + [summed(h, 0, 1, F32) for h in downs[2:]]
    gate_grad, up_grad, down_grad = kernel(
        finish_body,
        (*bases, last_a, last_b),
        [((d // BLOCKS, ff), BF16), ((d // BLOCKS, ff), BF16), ((ff // BLOCKS, d), BF16)],
        4,
        1 << 20,
    )

    side_rows = moved(side_rows, "c", 1)
    far_rows = (far_rows.astype(F32) + side_rows[PIECE:].astype(F32)).astype(BF16)
    far_rows = moved(far_rows, "zl", 1)
    input_grad, combine_grad = kernel(
        tokens_body, (expert_ids.T, own_rows, side_rows, far_rows), [((PIECE, d), BF16), ((2, PIECE), F32)], 8, 1 << 20
    )
    combine_grad = combine_grad.T
    return (input_grad, combine_grad, gate_grad[None], up_grad[None], down_grad[None])


def solution(mesh):
    torus = Mesh(mesh.devices.reshape(4, 2, 4, 2, 2), EVERY)
    tokens, weights, grads = P(EVERY, None), P(GROUP, None, None), P(GROUP, REPLICA, None)

    return jax.shard_map(
        shards,
        mesh=torus,
        in_specs=(tokens, tokens, tokens, tokens, weights, weights, weights),
        out_specs=(tokens, tokens, grads, grads, grads),
        check_vma=False,
    )
```

```python
import jax
import jax.numpy as jnp
from jax import lax
from jax.experimental import pallas as pl
from jax.experimental.pallas import tpu as pltpu
from jax.sharding import Mesh
from jax.sharding import PartitionSpec as P


F32 = jnp.float32
BF16 = jnp.bfloat16
GROUP = ("zl", "c")
REPLICA = ("x", "zh", "y")
EVERY = ("x", "zh", "y", "zl", "c")
XA, XB, YA, YB, Z = ("x", 1), ("x", 3), ("y", 1), ("y", 3), ("zh", 1)
ORDERS = ((XA, XB, YA, YB, Z), (YA, YB, XA, XB, Z), (XB, XA, YB, YA, Z), (YB, YA, XB, XA, Z))
DOWN_ORDERS = ORDERS[:2] + ((Z, XA, YB, YA, XB), (Z, YA, XB, XA, YB))
CHAINS = (2, 3, 0, 1)
BLOCKS = 32
HALF = BLOCKS // 2
PIECE = 128
LANES = 128
ROW = ((8, LANES), F32)


def moved(array, axis, mask):
    return lax.ppermute(array, axis, [(i, i ^ mask) for i in range(lax.axis_size(axis))])


def block_at(order, pos):
    masks = dict.fromkeys(REPLICA, 0)
    for step, (axis, mask) in enumerate(order):
        if pos >> (4 - step) & 1:
            masks[axis] ^= mask
    x, z, y = (lax.axis_index(axis) ^ masks[axis] for axis in REPLICA)
    return (x * 2 + z) * 4 + y


def group_index():
    return lax.axis_index("zl") * 2 + lax.axis_index("c")


def as_row(column):
    return jnp.broadcast_to(column, (column.shape[0], LANES)).T[:8]


def as_column(row):
    return jnp.broadcast_to(row[0:1, :], (LANES, LANES)).T[:, 0:1]


def nt(a, b):
    return lax.dot_general(a, b, (((1,), (1,)), ((), ())), preferred_element_type=F32)


def nn(a, b):
    return jnp.dot(a, b, preferred_element_type=F32)


def kernel(body, ins, outs, limit, flops, scratch=()):
    vmem = pl.BlockSpec(memory_space=pltpu.VMEM)
    return pl.pallas_call(
        body,
        in_specs=[vmem] * len(ins),
        out_specs=[vmem] * len(outs),
        out_shape=[jax.ShapeDtypeStruct(s, t) for s, t in outs],
        scratch_shapes=list(scratch),
        compiler_params=pltpu.CompilerParams(vmem_limit_bytes=limit << 20),
        cost_estimate=pl.CostEstimate(flops=flops, transcendentals=0, bytes_accessed=1 << 20),
    )(*ins)


def route_body(ids, combine, *outs):
    mine = group_index()
    for m, out in enumerate(outs):
        chosen = ids[...] == (mine ^ m)
        row = jnp.sum(jnp.where(chosen, combine[...], 0.0), axis=0, keepdims=True)
        out[...] = jnp.broadcast_to(row, out.shape)


def forward_body(x0, x1, c0, c1, wg, wu, slope, act_out, hid, cht, xt, xs):
    cw = jnp.concatenate([as_column(c0[...]), as_column(c1[...])], axis=0)
    for j, x in enumerate((x0, x1)):
        xs[pl.ds(j * PIECE, PIECE), :] = x[...]
    tile = 256
    for f in range(wg.shape[1] // tile):
        at = pl.ds(f * tile, tile)
        gate = nn(xs[...], wg[:, at])
        up = nn(xs[...], wu[:, at])
        sig = jax.nn.sigmoid(gate)
        act = gate * sig
        slope[:, at] = up * (sig * (1.0 + gate * (1.0 - sig)))
        act_out[:, at] = act
        hidden = act * up
        hid[:, at] = hidden.astype(BF16)
        cht[at, :] = (cw * hidden).T
    for j in range(2):
        xt[:, pl.ds(j * PIECE, PIECE)] = xs[pl.ds(j * PIECE, PIECE), :].T


def forward(x0, x1, cws, wg, wu):
    d, ff = wg.shape
    rows = 2 * PIECE
    outs = [((rows, ff), F32), ((rows, ff), F32), ((rows, ff), BF16), ((ff, rows), F32), ((d, rows), BF16)]
    return kernel(
        forward_body, (x0, x1, *cws, wg, wu), outs, 12, 4 * rows * d * ff, scratch=(pltpu.VMEM((rows, d), BF16),)
    )


def down_body(first, chunk, hta, htb, g0, g1, g2, g3, *refs):
    outs, (mixed, gs) = refs[:-2], refs[-2:]
    cols = g2.shape[1] // 2
    for j, g in enumerate((g0, g1)):
        gs[pl.ds(j * PIECE, PIECE), :] = g[:, pl.ds(chunk * 2 * cols, 2 * cols)]
    for j, g in enumerate((g2, g3)):
        gs[pl.ds((2 + j) * PIECE, PIECE), :] = g[...]
    size = hta.shape[0] // BLOCKS
    rows = hta.shape[1]
    for q in range(2):
        out = outs[q % len(outs)]
        base = q * (out.shape[0] // 2) if len(outs) == 1 else 0
        for b in range(HALF):
            start = pl.multiple_of(block_at(DOWN_ORDERS[2 * chunk + q], first + b) * size, 8)
            mixed[q, pl.ds(b * size, size), pl.ds(0, rows)] = hta[pl.ds(start, size), :]
            mixed[q, pl.ds(b * size, size), pl.ds(rows, rows)] = htb[pl.ds(start, size), :]
        part = nn(mixed[q].astype(BF16), gs[:, pl.ds(q * cols, cols)])
        for b in range(HALF):
            block = part[b * size : (b + 1) * size]
            stack = [block[:, k * LANES : (k + 1) * LANES] for k in range(cols // LANES)]
            tall = size * len(stack)
            out[pl.ds(base + b * tall, tall), :] = jnp.concatenate(stack, axis=0).astype(BF16)


def down_half(first, chunk, hts, pieces, joint=False):
    ff, rows = hts[0].shape
    width = pieces[2].shape[1]
    count = 1 if joint else 2
    out = ((2 // count * HALF * ff // BLOCKS * (width // 2 // LANES), LANES), BF16)

    def body(*refs):
        down_body(first, chunk, *refs)

    return kernel(
        body,
        (*hts, *pieces),
        [out] * count,
        12,
        2 * rows * ff * width,
        scratch=(pltpu.VMEM((2, ff // 2, 2 * rows), F32), pltpu.VMEM((2 * rows, width), BF16)),
    )


def hidden_body(pieces, c0, c1, wd, slope, act, hid, gd, ud, comb0, comb1, gs):
    cw = jnp.concatenate([as_column(c0[...]), as_column(c1[...])], axis=0)
    for j, chunks in enumerate(pieces):
        at = 0
        for g in chunks:
            gs[pl.ds(j * PIECE, PIECE), pl.ds(at, g.shape[1])] = g[...]
            at += g.shape[1]
    tile = 256
    total = jnp.zeros((gs.shape[0], 1), F32)
    for f in range(wd.shape[0] // tile):
        at = pl.ds(f * tile, tile)
        back = nt(gs[...], wd[at, :])
        total = total + jnp.sum(hid[:, at].astype(F32) * back, axis=1, keepdims=True)
        back = cw * back
        gd[:, at] = (back * slope[:, at]).astype(BF16)
        ud[:, at] = (back * act[:, at]).astype(BF16)
    comb0[...] = as_row(total[:PIECE])
    comb1[...] = as_row(total[PIECE:])


def hidden_part(pieces, cws, wd, slope, act, hid):
    ff, d = wd.shape
    rows = 2 * PIECE
    counts = [len(chunks) for chunks in pieces]

    def body(*refs):
        first, second = refs[: counts[0]], refs[counts[0] : sum(counts)]
        hidden_body((first, second), *refs[sum(counts) :])

    return kernel(
        body,
        (*pieces[0], *pieces[1], *cws, wd, slope, act, hid),
        [((rows, ff), BF16), ((rows, ff), BF16), ROW, ROW],
        10,
        2 * rows * d * ff,
        scratch=(pltpu.VMEM((rows, d), BF16),),
    )


TILE = 256
EARLY = ((2, 0, 3), (3, 0, 3))
LATER = ((0, 0, 3), (1, 0, 3))
EXTRA = 128


def gate_body(first, specs, xta, xtb, gda, gdb, uda, udb, *refs):
    outs, mixed = refs[:-1], refs[-1]
    size = xta.shape[0] // BLOCKS // 2
    rows = xta.shape[1]
    chains = []
    for (p, low, high), out in zip(specs, outs):
        if p not in chains:
            chains.append(p)
            at = chains.index(p)
            for b in range(HALF):
                start = pl.multiple_of(block_at(ORDERS[p], first + b) * (2 * size) + (p % 2) * size, size)
                mixed[at, pl.ds(b * size, size), pl.ds(0, rows)] = xta[pl.ds(start, size), :]
                mixed[at, pl.ds(b * size, size), pl.ds(rows, rows)] = xtb[pl.ds(start, size), :]
        q = chains.index(p)
        ga, gb = (gda, gdb) if p < 2 else (uda, udb)
        per = TILE // LANES
        tall = size * per * (high - low)
        for n in range(low, high):
            at = pl.ds(n * TILE, TILE)
            part = nn(mixed[q, :, pl.ds(0, rows)], ga[:, at]) + nn(mixed[q, :, pl.ds(rows, rows)], gb[:, at])
            part = part.astype(BF16)
            for b in range(HALF):
                for k in range(per):
                    to = b * tall + ((n - low) * per + k) * size
                    out[pl.ds(to, size), :] = part[b * size : (b + 1) * size, k * LANES : (k + 1) * LANES]


def gate_half(first, specs, xts, gds, uds):
    d, rows = xts[0].shape
    tiles = [high - low for _, low, high in specs]
    outs = [((HALF * (d // BLOCKS // 2) * t * (TILE // LANES), LANES), BF16) for t in tiles]

    def body(*refs):
        gate_body(first, specs, *refs)

    return kernel(
        body,
        (*xts, *gds, *uds),
        outs,
        12,
        d * rows * TILE * sum(tiles),
        scratch=(pltpu.VMEM((len({p for p, _, _ in specs}), d // 4, 2 * rows), BF16),),
    )


def rows_body(gda, gdb, uda, udb, wg, wu, *refs):
    combs, (own, side, across, gd, ud) = refs[:4], refs[4:]
    half = gda.shape[0]
    for scratch, pair in ((gd, (gda, gdb)), (ud, (uda, udb))):
        for j, ref in enumerate(pair):
            scratch[pl.ds(j * half, half), :] = ref[...]
    places = ((own, 0), (side, 0), (across, 0), (side, PIECE))
    tile = 512
    for n in range(wg.shape[0] // tile):
        at = pl.ds(n * tile, tile)
        total = (nt(gd[...], wg[at, :]) + nt(ud[...], wu[at, :])).astype(BF16)
        for j, (out, row) in enumerate(places):
            out[pl.ds(row, PIECE), at] = total[j * PIECE : (j + 1) * PIECE, :]
    mine = lax.broadcasted_iota(jnp.int32, (PIECE, EXTRA), 1) == group_index()
    for comb, (out, row) in zip(combs, places):
        value = jnp.where(mine, as_column(comb[...]), 0.0)
        out[pl.ds(row, PIECE), pl.ds(wg.shape[0], EXTRA)] = value.astype(BF16)


def tokens_body(ids, own, side, across, grad, combine):
    total = own[...].astype(F32) + side[pl.ds(0, PIECE), :].astype(F32) + across[...].astype(F32)
    d = grad.shape[1]
    grad[...] = total[:, :d].astype(BF16)
    lanes = total[:, d:].T
    picked = jnp.zeros(combine.shape, F32)
    for e in range(4):
        picked = picked + jnp.where(ids[...] == e, lanes[e : e + 1, :], 0.0)
    combine[...] = picked


def finish_body(*refs):
    bases, (last_a, last_b, end2, end3), (gate, up, down) = refs[:8], refs[8:12], refs[12:]
    half, low = gate.shape[0] // 2, down.shape[0]
    cols = down.shape[1] // 4
    received = [r[...].astype(F32) for r in (last_a, last_b, end2, end3)]
    received = jnp.concatenate(received, axis=0)
    done, at = [], 0
    for base in bases:
        done.append(base[...] + received[at : at + base.shape[0]])
        at += base.shape[0]
    for (p, first, _), total in zip(EARLY + LATER, done):
        out = gate if p < 2 else up
        for k in range(total.shape[0] // half):
            to = first * TILE + k * LANES
            out[pl.ds(p % 2 * half, half), pl.ds(to, LANES)] = total[k * half : (k + 1) * half].astype(BF16)
    for p, total in enumerate(done[4:]):
        for k in range(cols // LANES):
            down[:, pl.ds(p * cols + k * LANES, LANES)] = total[k * low : (k + 1) * low].astype(BF16)


def summed(arrays, start, stop, kind=BF16):
    total = 0.0
    for blocks, a in arrays:
        size = a.shape[0] // blocks
        total = total + a[start * size : stop * size].astype(F32)
    return total.astype(kind)


def shards(tokens, cotangent, expert_ids, combine, w_gate, w_up, w_down):
    wg, wu, wd = w_gate[0], w_up[0], w_down[0]
    d, ff = wg.shape
    rows = 4 * PIECE

    tok_far = moved(tokens, "zl", 1)
    tok_near = moved(tokens, "c", 1)
    own = kernel(route_body, (expert_ids.T, combine.T), [ROW] * 4, 2, 1 << 10)
    cws = [own[0]] + [moved(own[m], GROUP, m) for m in (1, 2, 3)]
    cwa, cwb = cws[:2], cws[2:]
    cot_near = moved(cotangent, "c", 1)
    cot_far = [moved(cotangent[:, k * d // 2 : (k + 1) * d // 2], "zl", 1) for k in range(2)]
    tok_both = moved(tok_far, "c", 1)
    cot_both = [moved(cot_far[k], "c", 1) for k in range(2)]

    fa = forward(tokens, tok_near, cwa, wg, wu)
    fb = forward(tok_far, tok_both, cwb, wg, wu)
    hts, xts = (fa[3], fb[3]), (fa[4], fb[4])
    pieces = [(cotangent, cot_near, cot_far[k], cot_both[k]) for k in range(2)]
    down_send = down_half(HALF, 0, hts, pieces[0])
    down_z = down_half(HALF, 1, hts, pieces[1], joint=True)[0]
    ha = hidden_part(((cotangent,), (cot_near,)), cwa, wd, *fa[:3])
    hb = hidden_part((cot_far, cot_both), cwb, wd, *fb[:3])
    gds, uds = (ha[0], hb[0]), (ha[1], hb[1])
    gate_send = list(gate_half(HALF, EARLY, xts, gds, uds))
    gate_send += gate_half(HALF, LATER, xts, gds, uds)
    down_keep = [a for k in range(2) for a in down_half(0, k, hts, pieces[k])]
    gate_keep = gate_half(0, EARLY + LATER, xts, gds, uds)
    own_rows, side_rows, far_rows = kernel(
        rows_body,
        (*gds, *uds, wg, wu, ha[2], ha[3], hb[2], hb[3]),
        [((n * PIECE, d + EXTRA), BF16) for n in (1, 2, 1)],
        12,
        4 * rows * d * ff,
        scratch=(pltpu.VMEM((rows, ff), BF16),) * 2,
    )

    down_z = moved(down_z, *Z)
    size = down_z.shape[0] // 2
    down_got = [moved(down_send[p], *ORDERS[p][0]) for p in (0, 1)]
    down_got += [lax.optimization_barrier(a) for a in (down_z[:size], down_z[size:])]
    gates, downs = [], [[(HALF, down_keep[p]), (HALF, down_got[p])] for p in range(4)]
    for spec, keep, send in zip(EARLY + LATER, gate_keep, gate_send):
        gates.append([(HALF, keep), (HALF, moved(send, *ORDERS[spec[0]][0]))])
    have = [[g for g, spec in zip(gates, EARLY + LATER) if spec[0] == p] + [downs[p]] for p in range(4)]
    left = {id(h): HALF for h in gates + downs}

    def exchange(held, step):
        sends = [summed(h, left[id(h)] // 2, left[id(h)]) for h in held]
        sent = jnp.concatenate(sends, axis=0)
        got = moved(sent, *step)
        at = 0
        for h, send in zip(held, sends):
            left[id(h)] //= 2
            h.append((left[id(h)], got[at : at + send.shape[0]]))
            at += send.shape[0]
        return got

    for p in CHAINS:
        exchange(have[p][: 2 if p < 2 else 1], ORDERS[p][1])
    for p in (2, 3):
        exchange(downs[p : p + 1], DOWN_ORDERS[p][1])
    for step in (2, 3):
        for p in CHAINS:
            exchange(have[p], ORDERS[p][step])
    last_a = exchange(gates[:2], Z)
    last_b = exchange(gates[2:] + downs[:2], Z)
    ends = [exchange(downs[p : p + 1], DOWN_ORDERS[p][4]) for p in (2, 3)]
    bases = [summed(h[:-1], 0, 1, F32) for h in gates + downs]
    gate_grad, up_grad, down_grad = kernel(
        finish_body,
        (*bases, last_a, last_b, *ends),
        [((d // BLOCKS, ff), BF16), ((d // BLOCKS, ff), BF16), ((ff // BLOCKS, d), BF16)],
        4,
        1 << 20,
    )

    side_rows = moved(side_rows, "c", 1)
    far_rows = (far_rows.astype(F32) + side_rows[PIECE:].astype(F32)).astype(BF16)
    far_rows = moved(far_rows, "zl", 1)
    input_grad, combine_grad = kernel(
        tokens_body, (expert_ids.T, own_rows, side_rows, far_rows), [((PIECE, d), BF16), ((2, PIECE), F32)], 8, 1 << 20
    )
    combine_grad = combine_grad.T
    return (input_grad, combine_grad, gate_grad[None], up_grad[None], down_grad[None])


def solution(mesh):
    torus = Mesh(mesh.devices.reshape(4, 2, 4, 2, 2), EVERY)
    tokens, weights, grads = P(EVERY, None), P(GROUP, None, None), P(GROUP, REPLICA, None)

    return jax.shard_map(
        shards,
        mesh=torus,
        in_specs=(tokens, tokens, tokens, tokens, weights, weights, weights),
        out_specs=(tokens, tokens, grads, grads, grads),
        check_vma=False,
    )
```

```python
import jax
import jax.numpy as jnp
from jax import lax
from jax.experimental import pallas as pl
from jax.experimental.pallas import tpu as pltpu
from jax.sharding import Mesh
from jax.sharding import PartitionSpec as P


F32 = jnp.float32
BF16 = jnp.bfloat16
GROUP = ("zl", "c")
REPLICA = ("x", "zh", "y")
EVERY = ("x", "zh", "y", "zl", "c")
XA, XB, YA, YB, Z = ("x", 1), ("x", 3), ("y", 1), ("y", 3), ("zh", 1)
ORDERS = ((XA, XB, YA, YB, Z), (YA, YB, XA, XB, Z), (XB, XA, YB, YA, Z), (YB, YA, XB, XA, Z))
DOWN_ORDERS = ORDERS[:2] + ((Z, XA, YB, YA, XB), (Z, YA, XB, XA, YB))
CHAINS = (2, 3, 0, 1)
BLOCKS = 32
HALF = BLOCKS // 2
PIECE = 128
LANES = 128
ROW = ((8, LANES), F32)


def moved(array, axis, mask):
    return lax.ppermute(array, axis, [(i, i ^ mask) for i in range(lax.axis_size(axis))])


def block_at(order, pos):
    masks = dict.fromkeys(REPLICA, 0)
    for step, (axis, mask) in enumerate(order):
        if pos >> (4 - step) & 1:
            masks[axis] ^= mask
    x, z, y = (lax.axis_index(axis) ^ masks[axis] for axis in REPLICA)
    return (x * 2 + z) * 4 + y


def group_index():
    return lax.axis_index("zl") * 2 + lax.axis_index("c")


def as_row(column):
    return jnp.broadcast_to(column, (column.shape[0], LANES)).T[:8]


def as_column(row):
    return jnp.broadcast_to(row[0:1, :], (LANES, LANES)).T[:, 0:1]


def nt(a, b):
    return lax.dot_general(a, b, (((1,), (1,)), ((), ())), preferred_element_type=F32)


def nn(a, b):
    return jnp.dot(a, b, preferred_element_type=F32)


def kernel(body, ins, outs, limit, flops, scratch=(), aliases=None):
    vmem = pl.BlockSpec(memory_space=pltpu.VMEM)
    return pl.pallas_call(
        body,
        in_specs=[vmem] * len(ins),
        out_specs=[vmem] * len(outs),
        out_shape=[jax.ShapeDtypeStruct(s, t) for s, t in outs],
        scratch_shapes=list(scratch),
        input_output_aliases=aliases or {},
        compiler_params=pltpu.CompilerParams(vmem_limit_bytes=limit << 20),
        cost_estimate=pl.CostEstimate(flops=flops, transcendentals=0, bytes_accessed=1 << 20),
    )(*ins)


def route_body(ids, combine, *outs):
    mine = group_index()
    for m, out in enumerate(outs):
        chosen = ids[...] == (mine ^ m)
        row = jnp.sum(jnp.where(chosen, combine[...], 0.0), axis=0, keepdims=True)
        out[...] = jnp.broadcast_to(row, out.shape)


def in_turn(body, ins, outs, limit, flops, scratch=()):
    def first(*refs):
        pl.when(lax.axis_index("c") != LEADER)(lambda: body(*refs))

    def second(*refs):
        kept = refs[: len(ins)] + refs[len(ins) + len(outs) :]
        pl.when(lax.axis_index("c") == LEADER)(lambda: body(*kept))

    early = kernel(first, ins, outs, limit, flops, scratch)
    aliases = {len(ins) + k: k for k in range(len(outs))}
    return kernel(second, (*ins, *early), outs, limit, flops, scratch, aliases)


def forward_body(x0, x1, c0, c1, wg, wu, slope, act_out, hid, cht, xt, xs):
    cw = jnp.concatenate([as_column(c0[...]), as_column(c1[...])], axis=0)
    for j, x in enumerate((x0, x1)):
        xs[pl.ds(j * PIECE, PIECE), :] = x[...]
    tile = 256
    for f in range(wg.shape[1] // tile):
        at = pl.ds(f * tile, tile)
        gate = nn(xs[...], wg[:, at])
        up = nn(xs[...], wu[:, at])
        sig = jax.nn.sigmoid(gate)
        act = gate * sig
        slope[:, at] = up * (sig * (1.0 + gate * (1.0 - sig)))
        act_out[:, at] = act
        hidden = act * up
        hid[:, at] = hidden.astype(BF16)
        cht[at, :] = (cw * hidden).T
    for j in range(2):
        xt[:, pl.ds(j * PIECE, PIECE)] = xs[pl.ds(j * PIECE, PIECE), :].T


def forward(x0, x1, cws, wg, wu):
    d, ff = wg.shape
    rows = 2 * PIECE
    outs = [((rows, ff), F32), ((rows, ff), F32), ((rows, ff), BF16), ((ff, rows), F32), ((d, rows), BF16)]
    return kernel(
        forward_body, (x0, x1, *cws, wg, wu), outs, 12, 4 * rows * d * ff, scratch=(pltpu.VMEM((rows, d), BF16),)
    )


def down_body(first, chunk, hta, htb, g0, g1, g2, g3, *refs):
    outs, (mixed, gs) = refs[:-2], refs[-2:]
    cols = g2.shape[1] // 2
    for j, g in enumerate((g0, g1)):
        gs[pl.ds(j * PIECE, PIECE), :] = g[:, pl.ds(chunk * 2 * cols, 2 * cols)]
    for j, g in enumerate((g2, g3)):
        gs[pl.ds((2 + j) * PIECE, PIECE), :] = g[...]
    size = hta.shape[0] // BLOCKS
    rows = hta.shape[1]
    for q in range(2):
        out = outs[q % len(outs)]
        base = q * (out.shape[0] // 2) if len(outs) == 1 else 0
        for b in range(HALF):
            start = pl.multiple_of(block_at(DOWN_ORDERS[2 * chunk + q], first + b) * size, 8)
            mixed[q, pl.ds(b * size, size), pl.ds(0, rows)] = hta[pl.ds(start, size), :]
            mixed[q, pl.ds(b * size, size), pl.ds(rows, rows)] = htb[pl.ds(start, size), :]
        part = nn(mixed[q].astype(BF16), gs[:, pl.ds(q * cols, cols)])
        for b in range(HALF):
            block = part[b * size : (b + 1) * size]
            stack = [block[:, k * LANES : (k + 1) * LANES] for k in range(cols // LANES)]
            tall = size * len(stack)
            out[pl.ds(base + b * tall, tall), :] = jnp.concatenate(stack, axis=0).astype(BF16)


def down_half(first, chunk, hts, pieces, joint=False):
    ff, rows = hts[0].shape
    width = pieces[2].shape[1]
    count = 1 if joint else 2
    out = ((2 // count * HALF * ff // BLOCKS * (width // 2 // LANES), LANES), BF16)

    def body(*refs):
        down_body(first, chunk, *refs)

    return kernel(
        body,
        (*hts, *pieces),
        [out] * count,
        12,
        2 * rows * ff * width,
        scratch=(pltpu.VMEM((2, ff // 2, 2 * rows), F32), pltpu.VMEM((2 * rows, width), BF16)),
    )


def hidden_body(pieces, c0, c1, wd, slope, act, hid, gd, ud, comb0, comb1, gs):
    cw = jnp.concatenate([as_column(c0[...]), as_column(c1[...])], axis=0)
    for j, chunks in enumerate(pieces):
        at = 0
        for g in chunks:
            gs[pl.ds(j * PIECE, PIECE), pl.ds(at, g.shape[1])] = g[...]
            at += g.shape[1]
    tile = 256
    total = jnp.zeros((gs.shape[0], 1), F32)
    for f in range(wd.shape[0] // tile):
        at = pl.ds(f * tile, tile)
        back = nt(gs[...], wd[at, :])
        total = total + jnp.sum(hid[:, at].astype(F32) * back, axis=1, keepdims=True)
        back = cw * back
        gd[:, at] = (back * slope[:, at]).astype(BF16)
        ud[:, at] = (back * act[:, at]).astype(BF16)
    comb0[...] = as_row(total[:PIECE])
    comb1[...] = as_row(total[PIECE:])


def hidden_part(pieces, cws, wd, slope, act, hid):
    ff, d = wd.shape
    rows = 2 * PIECE
    counts = [len(chunks) for chunks in pieces]

    def body(*refs):
        first, second = refs[: counts[0]], refs[counts[0] : sum(counts)]
        hidden_body((first, second), *refs[sum(counts) :])

    return kernel(
        body,
        (*pieces[0], *pieces[1], *cws, wd, slope, act, hid),
        [((rows, ff), BF16), ((rows, ff), BF16), ROW, ROW],
        10,
        2 * rows * d * ff,
        scratch=(pltpu.VMEM((rows, d), BF16),),
    )


TILE = 256
EARLY = ((2, 0, 3), (3, 0, 3))
LATER = ((0, 0, 3), (1, 0, 3))
LEADER = 1
EXTRA = 128


def gate_body(first, specs, xta, xtb, gda, gdb, uda, udb, *refs):
    outs, mixed = refs[:-1], refs[-1]
    size = xta.shape[0] // BLOCKS // 2
    rows = xta.shape[1]
    chains = []
    for (p, low, high), out in zip(specs, outs):
        if p not in chains:
            chains.append(p)
            at = chains.index(p)
            for b in range(HALF):
                start = pl.multiple_of(block_at(ORDERS[p], first + b) * (2 * size) + (p % 2) * size, size)
                mixed[at, pl.ds(b * size, size), pl.ds(0, rows)] = xta[pl.ds(start, size), :]
                mixed[at, pl.ds(b * size, size), pl.ds(rows, rows)] = xtb[pl.ds(start, size), :]
        q = chains.index(p)
        ga, gb = (gda, gdb) if p < 2 else (uda, udb)
        per = TILE // LANES
        tall = size * per * (high - low)
        for n in range(low, high):
            at = pl.ds(n * TILE, TILE)
            part = nn(mixed[q, :, pl.ds(0, rows)], ga[:, at]) + nn(mixed[q, :, pl.ds(rows, rows)], gb[:, at])
            part = part.astype(BF16)
            for b in range(HALF):
                for k in range(per):
                    to = b * tall + ((n - low) * per + k) * size
                    out[pl.ds(to, size), :] = part[b * size : (b + 1) * size, k * LANES : (k + 1) * LANES]


def gate_half(first, specs, xts, gds, uds):
    d, rows = xts[0].shape
    tiles = [high - low for _, low, high in specs]
    outs = [((HALF * (d // BLOCKS // 2) * t * (TILE // LANES), LANES), BF16) for t in tiles]

    def body(*refs):
        gate_body(first, specs, *refs)

    return kernel(
        body,
        (*xts, *gds, *uds),
        outs,
        12,
        d * rows * TILE * sum(tiles),
        scratch=(pltpu.VMEM((len({p for p, _, _ in specs}), d // 4, 2 * rows), BF16),),
    )


def rows_body(gda, gdb, uda, udb, wg, wu, *refs):
    combs, (own, side, across, gd, ud) = refs[:4], refs[4:]
    half = gda.shape[0]
    for scratch, pair in ((gd, (gda, gdb)), (ud, (uda, udb))):
        for j, ref in enumerate(pair):
            scratch[pl.ds(j * half, half), :] = ref[...]
    places = ((own, 0), (side, 0), (across, 0), (side, PIECE))
    tile = 512
    for n in range(wg.shape[0] // tile):
        at = pl.ds(n * tile, tile)
        total = (nt(gd[...], wg[at, :]) + nt(ud[...], wu[at, :])).astype(BF16)
        for j, (out, row) in enumerate(places):
            out[pl.ds(row, PIECE), at] = total[j * PIECE : (j + 1) * PIECE, :]
    mine = lax.broadcasted_iota(jnp.int32, (PIECE, EXTRA), 1) == group_index()
    for comb, (out, row) in zip(combs, places):
        value = jnp.where(mine, as_column(comb[...]), 0.0)
        out[pl.ds(row, PIECE), pl.ds(wg.shape[0], EXTRA)] = value.astype(BF16)


def tokens_body(ids, own, side, across, grad, combine):
    total = own[...].astype(F32) + side[pl.ds(0, PIECE), :].astype(F32) + across[...].astype(F32)
    d = grad.shape[1]
    grad[...] = total[:, :d].astype(BF16)
    lanes = total[:, d:].T
    picked = jnp.zeros(combine.shape, F32)
    for e in range(4):
        picked = picked + jnp.where(ids[...] == e, lanes[e : e + 1, :], 0.0)
    combine[...] = picked


def finish_body(*refs):
    bases, (last_a, last_b, end2, end3), (gate, up, down) = refs[:8], refs[8:12], refs[12:]
    half, low = gate.shape[0] // 2, down.shape[0]
    cols = down.shape[1] // 4
    received = [r[...].astype(F32) for r in (last_a, last_b, end2, end3)]
    received = jnp.concatenate(received, axis=0)
    done, at = [], 0
    for base in bases:
        done.append(base[...] + received[at : at + base.shape[0]])
        at += base.shape[0]
    for (p, first, _), total in zip(EARLY + LATER, done):
        out = gate if p < 2 else up
        for k in range(total.shape[0] // half):
            to = first * TILE + k * LANES
            out[pl.ds(p % 2 * half, half), pl.ds(to, LANES)] = total[k * half : (k + 1) * half].astype(BF16)
    for p, total in enumerate(done[4:]):
        for k in range(cols // LANES):
            down[:, pl.ds(p * cols + k * LANES, LANES)] = total[k * low : (k + 1) * low].astype(BF16)


def summed(arrays, start, stop, kind=BF16):
    total = 0.0
    for blocks, a in arrays:
        size = a.shape[0] // blocks
        total = total + a[start * size : stop * size].astype(F32)
    return total.astype(kind)


def shards(tokens, cotangent, expert_ids, combine, w_gate, w_up, w_down):
    wg, wu, wd = w_gate[0], w_up[0], w_down[0]
    d, ff = wg.shape
    rows = 4 * PIECE

    tok_far = moved(tokens, "zl", 1)
    tok_near = moved(tokens, "c", 1)
    own = kernel(route_body, (expert_ids.T, combine.T), [ROW] * 4, 2, 1 << 10)
    cws = [own[0]] + [moved(own[m], GROUP, m) for m in (1, 2, 3)]
    cwa, cwb = cws[:2], cws[2:]
    cot_near = moved(cotangent, "c", 1)
    cot_far = [moved(cotangent[:, k * d // 2 : (k + 1) * d // 2], "zl", 1) for k in range(2)]
    tok_both = moved(tok_far, "c", 1)
    cot_both = [moved(cot_far[k], "c", 1) for k in range(2)]

    fa = forward(tokens, tok_near, cwa, wg, wu)
    fb = forward(tok_far, tok_both, cwb, wg, wu)
    hts, xts = (fa[3], fb[3]), (fa[4], fb[4])
    pieces = [(cotangent, cot_near, cot_far[k], cot_both[k]) for k in range(2)]
    down_send = down_half(HALF, 0, hts, pieces[0])
    down_z = down_half(HALF, 1, hts, pieces[1], joint=True)[0]
    ha = hidden_part(((cotangent,), (cot_near,)), cwa, wd, *fa[:3])
    hb = hidden_part((cot_far, cot_both), cwb, wd, *fb[:3])
    gds, uds = (ha[0], hb[0]), (ha[1], hb[1])
    gate_send = list(gate_half(HALF, EARLY, xts, gds, uds))
    gate_send += gate_half(HALF, LATER, xts, gds, uds)
    down_keep = [a for k in range(2) for a in down_half(0, k, hts, pieces[k])]
    gate_keep = gate_half(0, EARLY + LATER, xts, gds, uds)
    own_rows, side_rows, far_rows = in_turn(
        rows_body,
        (*gds, *uds, wg, wu, ha[2], ha[3], hb[2], hb[3]),
        [((n * PIECE, d + EXTRA), BF16) for n in (1, 2, 1)],
        12,
        4 * rows * d * ff,
        scratch=(pltpu.VMEM((rows, ff), BF16),) * 2,
    )

    down_z = moved(down_z, *Z)
    size = down_z.shape[0] // 2
    down_got = [moved(down_send[p], *ORDERS[p][0]) for p in (0, 1)]
    down_got += [lax.optimization_barrier(a) for a in (down_z[:size], down_z[size:])]
    gates, downs = [], [[(HALF, down_keep[p]), (HALF, down_got[p])] for p in range(4)]
    for spec, keep, send in zip(EARLY + LATER, gate_keep, gate_send):
        gates.append([(HALF, keep), (HALF, moved(send, *ORDERS[spec[0]][0]))])
    have = [[g for g, spec in zip(gates, EARLY + LATER) if spec[0] == p] + [downs[p]] for p in range(4)]
    left = {id(h): HALF for h in gates + downs}

    def exchange(held, step):
        sends = [summed(h, left[id(h)] // 2, left[id(h)]) for h in held]
        sent = jnp.concatenate(sends, axis=0)
        got = moved(sent, *step)
        at = 0
        for h, send in zip(held, sends):
            left[id(h)] //= 2
            h.append((left[id(h)], got[at : at + send.shape[0]]))
            at += send.shape[0]
        return got

    for p in CHAINS:
        exchange(have[p][: 2 if p < 2 else 1], ORDERS[p][1])
    for p in (2, 3):
        exchange(downs[p : p + 1], DOWN_ORDERS[p][1])
    for step in (2, 3):
        for p in CHAINS:
            exchange(have[p], ORDERS[p][step])
    last_a = exchange(gates[:2], Z)
    last_b = exchange(gates[2:] + downs[:2], Z)
    ends = [exchange(downs[p : p + 1], DOWN_ORDERS[p][4]) for p in (2, 3)]
    bases = [summed(h[:-1], 0, 1, F32) for h in gates + downs]
    gate_grad, up_grad, down_grad = kernel(
        finish_body,
        (*bases, last_a, last_b, *ends),
        [((d // BLOCKS, ff), BF16), ((d // BLOCKS, ff), BF16), ((ff // BLOCKS, d), BF16)],
        4,
        1 << 20,
    )

    side_rows = moved(side_rows, "c", 1)
    far_rows = (far_rows.astype(F32) + side_rows[PIECE:].astype(F32)).astype(BF16)
    far_rows = moved(far_rows, "zl", 1)
    input_grad, combine_grad = kernel(
        tokens_body, (expert_ids.T, own_rows, side_rows, far_rows), [((PIECE, d), BF16), ((2, PIECE), F32)], 8, 1 << 20
    )
    combine_grad = combine_grad.T
    return (input_grad, combine_grad, gate_grad[None], up_grad[None], down_grad[None])


def solution(mesh):
    torus = Mesh(mesh.devices.reshape(4, 2, 4, 2, 2), EVERY)
    tokens, weights, grads = P(EVERY, None), P(GROUP, None, None), P(GROUP, REPLICA, None)

    return jax.shard_map(
        shards,
        mesh=torus,
        in_specs=(tokens, tokens, tokens, tokens, weights, weights, weights),
        out_specs=(tokens, tokens, grads, grads, grads),
        check_vma=False,
    )
```

```python
import jax
import jax.numpy as jnp
from jax import lax
from jax.experimental import pallas as pl
from jax.experimental.pallas import tpu as pltpu
from jax.sharding import Mesh
from jax.sharding import PartitionSpec as P


F32 = jnp.float32
BF16 = jnp.bfloat16
GROUP = ("zl", "c")
REPLICA = ("x", "zh", "y")
EVERY = ("x", "zh", "y", "zl", "c")
XA, XB, YA, YB, Z = ("x", 1), ("x", 3), ("y", 1), ("y", 3), ("zh", 1)
ORDERS = ((XA, XB, YA, YB, Z), (YA, YB, XA, XB, Z), (XB, XA, YB, YA, Z), (YB, YA, XB, XA, Z))
CHAINS = (0, 1, 2, 3)
BLOCKS = 32
HALF = BLOCKS // 2
PIECE = 128
LANES = 128
ROW = ((8, LANES), F32)


def moved(array, axis, mask):
    return lax.ppermute(array, axis, [(i, i ^ mask) for i in range(lax.axis_size(axis))])


def block_at(order, pos):
    masks = dict.fromkeys(REPLICA, 0)
    for step, (axis, mask) in enumerate(order):
        if pos >> (4 - step) & 1:
            masks[axis] ^= mask
    x, z, y = (lax.axis_index(axis) ^ masks[axis] for axis in REPLICA)
    return (x * 2 + z) * 4 + y


def group_index():
    return lax.axis_index("zl") * 2 + lax.axis_index("c")


def as_row(column):
    return jnp.broadcast_to(column, (column.shape[0], LANES)).T[:8]


def as_column(row):
    return jnp.broadcast_to(row[0:1, :], (LANES, LANES)).T[:, 0:1]


def nt(a, b):
    return lax.dot_general(a, b, (((1,), (1,)), ((), ())), preferred_element_type=F32)


def nn(a, b):
    return jnp.dot(a, b, preferred_element_type=F32)


def kernel(body, ins, outs, limit, flops, scratch=()):
    vmem = pl.BlockSpec(memory_space=pltpu.VMEM)
    return pl.pallas_call(
        body,
        in_specs=[vmem] * len(ins),
        out_specs=[vmem] * len(outs),
        out_shape=[jax.ShapeDtypeStruct(s, t) for s, t in outs],
        scratch_shapes=list(scratch),
        compiler_params=pltpu.CompilerParams(vmem_limit_bytes=limit << 20),
        cost_estimate=pl.CostEstimate(flops=flops, transcendentals=0, bytes_accessed=1 << 20),
    )(*ins)


def route_body(ids, combine, *outs):
    mine = group_index()
    for m, out in enumerate(outs):
        chosen = ids[...] == (mine ^ m)
        row = jnp.sum(jnp.where(chosen, combine[...], 0.0), axis=0, keepdims=True)
        out[...] = jnp.broadcast_to(row, out.shape)


def forward_body(x0, x1, c0, c1, wg, wu, slope, act_out, hid, cht, xt, xs):
    cw = jnp.concatenate([as_column(c0[...]), as_column(c1[...])], axis=0)
    for j, x in enumerate((x0, x1)):
        xs[pl.ds(j * PIECE, PIECE), :] = x[...]
    tile = 256
    for f in range(wg.shape[1] // tile):
        at = pl.ds(f * tile, tile)
        gate = nn(xs[...], wg[:, at])
        up = nn(xs[...], wu[:, at])
        sig = jax.nn.sigmoid(gate)
        act = gate * sig
        slope[:, at] = up * (sig * (1.0 + gate * (1.0 - sig)))
        act_out[:, at] = act
        hidden = act * up
        hid[:, at] = hidden.astype(BF16)
        cht[at, :] = (cw * hidden).T
    for j in range(2):
        xt[:, pl.ds(j * PIECE, PIECE)] = xs[pl.ds(j * PIECE, PIECE), :].T


def forward(x0, x1, cws, wg, wu):
    d, ff = wg.shape
    rows = 2 * PIECE
    outs = [((rows, ff), F32), ((rows, ff), F32), ((rows, ff), BF16), ((ff, rows), F32), ((d, rows), BF16)]
    return kernel(
        forward_body, (x0, x1, *cws, wg, wu), outs, 12, 4 * rows * d * ff, scratch=(pltpu.VMEM((rows, d), BF16),)
    )


def down_body(first, chunk, hta, htb, g0, g1, g2, g3, *refs):
    outs, (mixed, gs) = refs[:-2], refs[-2:]
    cols = g2.shape[1] // 2
    for j, g in enumerate((g0, g1)):
        gs[pl.ds(j * PIECE, PIECE), :] = g[:, pl.ds(chunk * 2 * cols, 2 * cols)]
    for j, g in enumerate((g2, g3)):
        gs[pl.ds((2 + j) * PIECE, PIECE), :] = g[...]
    size = hta.shape[0] // BLOCKS
    rows = hta.shape[1]
    for q in range(2):
        out = outs[q]
        for b in range(HALF):
            start = pl.multiple_of(block_at(ORDERS[2 * chunk + q], first + b) * size, 8)
            mixed[q, pl.ds(b * size, size), pl.ds(0, rows)] = hta[pl.ds(start, size), :]
            mixed[q, pl.ds(b * size, size), pl.ds(rows, rows)] = htb[pl.ds(start, size), :]
        part = nn(mixed[q].astype(BF16), gs[:, pl.ds(q * cols, cols)])
        for b in range(HALF):
            block = part[b * size : (b + 1) * size]
            stack = [block[:, k * LANES : (k + 1) * LANES] for k in range(cols // LANES)]
            tall = size * len(stack)
            out[pl.ds(b * tall, tall), :] = jnp.concatenate(stack, axis=0).astype(BF16)


def down_half(first, chunk, hts, pieces):
    ff, rows = hts[0].shape
    width = pieces[2].shape[1]
    out = ((HALF * ff // BLOCKS * (width // 2 // LANES), LANES), BF16)

    def body(*refs):
        down_body(first, chunk, *refs)

    return kernel(
        body,
        (*hts, *pieces),
        [out] * 2,
        12,
        2 * rows * ff * width,
        scratch=(pltpu.VMEM((2, ff // 2, 2 * rows), F32), pltpu.VMEM((2 * rows, width), BF16)),
    )


def hidden_body(pieces, c0, c1, wd, slope, act, hid, gd, ud, comb0, comb1, gs):
    cw = jnp.concatenate([as_column(c0[...]), as_column(c1[...])], axis=0)
    for j, chunks in enumerate(pieces):
        at = 0
        for g in chunks:
            gs[pl.ds(j * PIECE, PIECE), pl.ds(at, g.shape[1])] = g[...]
            at += g.shape[1]
    tile = 256
    total = jnp.zeros((gs.shape[0], 1), F32)
    for f in range(wd.shape[0] // tile):
        at = pl.ds(f * tile, tile)
        back = nt(gs[...], wd[at, :])
        total = total + jnp.sum(hid[:, at].astype(F32) * back, axis=1, keepdims=True)
        back = cw * back
        gd[:, at] = (back * slope[:, at]).astype(BF16)
        ud[:, at] = (back * act[:, at]).astype(BF16)
    comb0[...] = as_row(total[:PIECE])
    comb1[...] = as_row(total[PIECE:])


def hidden_part(pieces, cws, wd, slope, act, hid):
    ff, d = wd.shape
    rows = 2 * PIECE
    counts = [len(chunks) for chunks in pieces]

    def body(*refs):
        first, second = refs[: counts[0]], refs[counts[0] : sum(counts)]
        hidden_body((first, second), *refs[sum(counts) :])

    return kernel(
        body,
        (*pieces[0], *pieces[1], *cws, wd, slope, act, hid),
        [((rows, ff), BF16), ((rows, ff), BF16), ROW, ROW],
        10,
        2 * rows * d * ff,
        scratch=(pltpu.VMEM((rows, d), BF16),),
    )


TILE = 256
EARLY = ((0, 0, 3), (1, 0, 3))
LATER = ((2, 0, 3), (3, 0, 3))
EXTRA = 128


def gate_body(first, specs, xta, xtb, gda, gdb, uda, udb, *refs):
    outs, mixed = refs[:-1], refs[-1]
    size = xta.shape[0] // BLOCKS // 2
    rows = xta.shape[1]
    chains = []
    for (p, low, high), out in zip(specs, outs):
        if p not in chains:
            chains.append(p)
            at = chains.index(p)
            for b in range(HALF):
                start = pl.multiple_of(block_at(ORDERS[p], first + b) * (2 * size) + (p % 2) * size, size)
                mixed[at, pl.ds(b * size, size), pl.ds(0, rows)] = xta[pl.ds(start, size), :]
                mixed[at, pl.ds(b * size, size), pl.ds(rows, rows)] = xtb[pl.ds(start, size), :]
        q = chains.index(p)
        ga, gb = (gda, gdb) if p < 2 else (uda, udb)
        per = TILE // LANES
        tall = size * per * (high - low)
        for n in range(low, high):
            at = pl.ds(n * TILE, TILE)
            part = nn(mixed[q, :, pl.ds(0, rows)], ga[:, at]) + nn(mixed[q, :, pl.ds(rows, rows)], gb[:, at])
            part = part.astype(BF16)
            for b in range(HALF):
                for k in range(per):
                    to = b * tall + ((n - low) * per + k) * size
                    out[pl.ds(to, size), :] = part[b * size : (b + 1) * size, k * LANES : (k + 1) * LANES]


def gate_half(first, specs, xts, gds, uds):
    d, rows = xts[0].shape
    tiles = [high - low for _, low, high in specs]
    outs = [((HALF * (d // BLOCKS // 2) * t * (TILE // LANES), LANES), BF16) for t in tiles]

    def body(*refs):
        gate_body(first, specs, *refs)

    return kernel(
        body,
        (*xts, *gds, *uds),
        outs,
        12,
        d * rows * TILE * sum(tiles),
        scratch=(pltpu.VMEM((len({p for p, _, _ in specs}), d // 4, 2 * rows), BF16),),
    )


def rows_body(gda, gdb, uda, udb, wg, wu, *refs):
    combs, (own, side, across, gd, ud) = refs[:4], refs[4:]
    half = gda.shape[0]
    for scratch, pair in ((gd, (gda, gdb)), (ud, (uda, udb))):
        for j, ref in enumerate(pair):
            scratch[pl.ds(j * half, half), :] = ref[...]
    places = ((own, 0), (side, 0), (across, 0), (side, PIECE))
    tile = 512
    for n in range(wg.shape[0] // tile):
        at = pl.ds(n * tile, tile)
        total = (nt(gd[...], wg[at, :]) + nt(ud[...], wu[at, :])).astype(BF16)
        for j, (out, row) in enumerate(places):
            out[pl.ds(row, PIECE), at] = total[j * PIECE : (j + 1) * PIECE, :]
    mine = lax.broadcasted_iota(jnp.int32, (PIECE, EXTRA), 1) == group_index()
    for comb, (out, row) in zip(combs, places):
        value = jnp.where(mine, as_column(comb[...]), 0.0)
        out[pl.ds(row, PIECE), pl.ds(wg.shape[0], EXTRA)] = value.astype(BF16)


def tokens_body(ids, own, side, across, grad, combine):
    total = own[...].astype(F32) + side[pl.ds(0, PIECE), :].astype(F32) + across[...].astype(F32)
    d = grad.shape[1]
    grad[...] = total[:, :d].astype(BF16)
    lanes = total[:, d:].T
    picked = jnp.zeros(combine.shape, F32)
    for e in range(4):
        picked = picked + jnp.where(ids[...] == e, lanes[e : e + 1, :], 0.0)
    combine[...] = picked


def finish_body(*refs):
    bases, last, (gate, up, down) = refs[:8], refs[8], refs[9:]
    half, low = gate.shape[0] // 2, down.shape[0]
    cols = down.shape[1] // 4
    received = last[...].astype(F32)
    done, at = [], 0
    for base in bases:
        done.append(base[...] + received[at : at + base.shape[0]])
        at += base.shape[0]
    for (p, first, _), total in zip(EARLY + LATER, done):
        out = gate if p < 2 else up
        for k in range(total.shape[0] // half):
            to = first * TILE + k * LANES
            out[pl.ds(p % 2 * half, half), pl.ds(to, LANES)] = total[k * half : (k + 1) * half].astype(BF16)
    for p, total in enumerate(done[4:]):
        for k in range(cols // LANES):
            down[:, pl.ds(p * cols + k * LANES, LANES)] = total[k * low : (k + 1) * low].astype(BF16)


def summed(arrays, start, stop, kind=BF16):
    total = 0.0
    for blocks, a in arrays:
        size = a.shape[0] // blocks
        total = total + a[start * size : stop * size].astype(F32)
    return total.astype(kind)


def shards(tokens, cotangent, expert_ids, combine, w_gate, w_up, w_down):
    wg, wu, wd = w_gate[0], w_up[0], w_down[0]
    d, ff = wg.shape
    rows = 4 * PIECE

    tok_far = moved(tokens, "zl", 1)
    tok_near = moved(tokens, "c", 1)
    own = kernel(route_body, (expert_ids.T, combine.T), [ROW] * 4, 2, 1 << 10)
    cws = [own[0]] + [moved(own[m], GROUP, m) for m in (1, 2, 3)]
    cwa, cwb = cws[:2], cws[2:]
    cot_near = moved(cotangent, "c", 1)
    cot_far = [moved(cotangent[:, k * d // 2 : (k + 1) * d // 2], "zl", 1) for k in range(2)]
    tok_both = moved(tok_far, "c", 1)
    cot_both = [moved(cot_far[k], "c", 1) for k in range(2)]

    fa = forward(tokens, tok_near, cwa, wg, wu)
    fb = forward(tok_far, tok_both, cwb, wg, wu)
    hts, xts = (fa[3], fb[3]), (fa[4], fb[4])
    pieces = [(cotangent, cot_near, cot_far[k], cot_both[k]) for k in range(2)]
    down_send = [a for k in range(2) for a in down_half(HALF, k, hts, pieces[k])]
    ha = hidden_part(((cotangent,), (cot_near,)), cwa, wd, *fa[:3])
    hb = hidden_part((cot_far, cot_both), cwb, wd, *fb[:3])
    gds, uds = (ha[0], hb[0]), (ha[1], hb[1])
    gate_send = list(gate_half(HALF, EARLY, xts, gds, uds))
    gate_send += gate_half(HALF, LATER, xts, gds, uds)
    down_keep = [a for k in range(2) for a in down_half(0, k, hts, pieces[k])]
    gate_keep = gate_half(0, EARLY + LATER, xts, gds, uds)
    own_rows, side_rows, far_rows = kernel(
        rows_body,
        (*gds, *uds, wg, wu, ha[2], ha[3], hb[2], hb[3]),
        [((n * PIECE, d + EXTRA), BF16) for n in (1, 2, 1)],
        12,
        4 * rows * d * ff,
        scratch=(pltpu.VMEM((rows, ff), BF16),) * 2,
    )

    down_got = [moved(down_send[p], *ORDERS[p][0]) for p in range(4)]
    gates, downs = [], [[(HALF, down_keep[p]), (HALF, down_got[p])] for p in range(4)]
    for spec, keep, send in zip(EARLY + LATER, gate_keep, gate_send):
        gates.append([(HALF, keep), (HALF, moved(send, *ORDERS[spec[0]][0]))])
    have = [[g for g, spec in zip(gates, EARLY + LATER) if spec[0] == p] + [downs[p]] for p in range(4)]
    left = {id(h): HALF for h in gates + downs}

    def exchange(held, step):
        sends = [summed(h, left[id(h)] // 2, left[id(h)]) for h in held]
        sent = jnp.concatenate(sends, axis=0)
        got = moved(sent, *step)
        at = 0
        for h, send in zip(held, sends):
            left[id(h)] //= 2
            h.append((left[id(h)], got[at : at + send.shape[0]]))
            at += send.shape[0]
        return got

    for step in (1, 2, 3):
        for p in CHAINS:
            exchange(have[p], ORDERS[p][step])
    last = exchange(gates + downs, Z)
    bases = [summed(h[:-1], 0, 1, F32) for h in gates + downs]
    gate_grad, up_grad, down_grad = kernel(
        finish_body,
        (*bases, last),
        [((d // BLOCKS, ff), BF16), ((d // BLOCKS, ff), BF16), ((ff // BLOCKS, d), BF16)],
        4,
        1 << 20,
    )

    side_rows = moved(side_rows, "c", 1)
    far_rows = (far_rows.astype(F32) + side_rows[PIECE:].astype(F32)).astype(BF16)
    far_rows = moved(far_rows, "zl", 1)
    input_grad, combine_grad = kernel(
        tokens_body, (expert_ids.T, own_rows, side_rows, far_rows), [((PIECE, d), BF16), ((2, PIECE), F32)], 8, 1 << 20
    )
    combine_grad = combine_grad.T
    return (input_grad, combine_grad, gate_grad[None], up_grad[None], down_grad[None])


def solution(mesh):
    torus = Mesh(mesh.devices.reshape(4, 2, 4, 2, 2), EVERY)
    tokens, weights, grads = P(EVERY, None), P(GROUP, None, None), P(GROUP, REPLICA, None)

    return jax.shard_map(
        shards,
        mesh=torus,
        in_specs=(tokens, tokens, tokens, tokens, weights, weights, weights),
        out_specs=(tokens, tokens, grads, grads, grads),
        check_vma=False,
    )
```

```python
import jax
import jax.numpy as jnp
from jax import lax
from jax.experimental import pallas as pl
from jax.experimental.pallas import tpu as pltpu
from jax.sharding import Mesh
from jax.sharding import PartitionSpec as P


F32 = jnp.float32
BF16 = jnp.bfloat16
GROUP = ("zl", "c")
REPLICA = ("x", "zh", "y")
EVERY = ("x", "zh", "y", "zl", "c")
XA, XB, YA, YB, Z = ("x", 1), ("x", 3), ("y", 1), ("y", 3), ("zh", 1)
ORDERS = ((XA, XB, YA, YB, Z), (YA, YB, XA, XB, Z), (XB, XA, YB, YA, Z), (YB, YA, XB, XA, Z))
CHAINS = (0, 1, 2, 3)
BLOCKS = 32
HALF = BLOCKS // 2
PIECE = 128
LANES = 128
ROW = ((8, LANES), F32)


def moved(array, axis, mask):
    return lax.ppermute(array, axis, [(i, i ^ mask) for i in range(lax.axis_size(axis))])


def block_at(order, pos):
    masks = dict.fromkeys(REPLICA, 0)
    for step, (axis, mask) in enumerate(order):
        if pos >> (4 - step) & 1:
            masks[axis] ^= mask
    x, z, y = (lax.axis_index(axis) ^ masks[axis] for axis in REPLICA)
    return (x * 2 + z) * 4 + y


def group_index():
    return lax.axis_index("zl") * 2 + lax.axis_index("c")


def as_row(column):
    return jnp.broadcast_to(column, (column.shape[0], LANES)).T[:8]


def as_column(row):
    return jnp.broadcast_to(row[0:1, :], (LANES, LANES)).T[:, 0:1]


def nt(a, b):
    return lax.dot_general(a, b, (((1,), (1,)), ((), ())), preferred_element_type=F32)


def nn(a, b):
    return jnp.dot(a, b, preferred_element_type=F32)


def kernel(body, ins, outs, limit, flops, scratch=()):
    vmem = pl.BlockSpec(memory_space=pltpu.VMEM)
    return pl.pallas_call(
        body,
        in_specs=[vmem] * len(ins),
        out_specs=[vmem] * len(outs),
        out_shape=[jax.ShapeDtypeStruct(s, t) for s, t in outs],
        scratch_shapes=list(scratch),
        compiler_params=pltpu.CompilerParams(vmem_limit_bytes=limit << 20),
        cost_estimate=pl.CostEstimate(flops=flops, transcendentals=0, bytes_accessed=1 << 20),
    )(*ins)


def route_body(ids, combine, *outs):
    mine = group_index()
    for m, out in enumerate(outs):
        chosen = ids[...] == (mine ^ m)
        row = jnp.sum(jnp.where(chosen, combine[...], 0.0), axis=0, keepdims=True)
        out[...] = jnp.broadcast_to(row, out.shape)


def forward_body(x0, x1, c0, c1, wg, wu, slope, act_out, hid, cht, xt, xs):
    cw = jnp.concatenate([as_column(c0[...]), as_column(c1[...])], axis=0)
    for j, x in enumerate((x0, x1)):
        xs[pl.ds(j * PIECE, PIECE), :] = x[...]
    tile = 256
    for f in range(wg.shape[1] // tile):
        at = pl.ds(f * tile, tile)
        gate = nn(xs[...], wg[:, at])
        up = nn(xs[...], wu[:, at])
        sig = jax.nn.sigmoid(gate)
        act = gate * sig
        slope[:, at] = up * (sig * (1.0 + gate * (1.0 - sig)))
        act_out[:, at] = act
        hidden = act * up
        hid[:, at] = hidden.astype(BF16)
        cht[at, :] = (cw * hidden).T
    for j in range(2):
        xt[:, pl.ds(j * PIECE, PIECE)] = xs[pl.ds(j * PIECE, PIECE), :].T


def forward(x0, x1, cws, wg, wu):
    d, ff = wg.shape
    rows = 2 * PIECE
    outs = [((rows, ff), F32), ((rows, ff), F32), ((rows, ff), BF16), ((ff, rows), F32), ((d, rows), BF16)]
    return kernel(
        forward_body, (x0, x1, *cws, wg, wu), outs, 12, 4 * rows * d * ff, scratch=(pltpu.VMEM((rows, d), BF16),)
    )


def down_body(first, chunk, hta, htb, g0, g1, g2, g3, *refs):
    outs, (mixed, gs) = refs[:-2], refs[-2:]
    cols = g2.shape[1] // 2
    for j, g in enumerate((g0, g1)):
        gs[pl.ds(j * PIECE, PIECE), :] = g[:, pl.ds(chunk * 2 * cols, 2 * cols)]
    for j, g in enumerate((g2, g3)):
        gs[pl.ds((2 + j) * PIECE, PIECE), :] = g[...]
    size = hta.shape[0] // BLOCKS
    rows = hta.shape[1]
    for q in range(2):
        out = outs[q]
        for b in range(HALF):
            start = pl.multiple_of(block_at(ORDERS[2 * chunk + q], first + b) * size, 8)
            mixed[q, pl.ds(b * size, size), pl.ds(0, rows)] = hta[pl.ds(start, size), :]
            mixed[q, pl.ds(b * size, size), pl.ds(rows, rows)] = htb[pl.ds(start, size), :]
        part = nn(mixed[q].astype(BF16), gs[:, pl.ds(q * cols, cols)])
        for b in range(HALF):
            block = part[b * size : (b + 1) * size]
            stack = [block[:, k * LANES : (k + 1) * LANES] for k in range(cols // LANES)]
            tall = size * len(stack)
            out[pl.ds(b * tall, tall), :] = jnp.concatenate(stack, axis=0).astype(BF16)


def down_half(first, chunk, hts, pieces):
    ff, rows = hts[0].shape
    width = pieces[2].shape[1]
    out = ((HALF * ff // BLOCKS * (width // 2 // LANES), LANES), BF16)

    def body(*refs):
        down_body(first, chunk, *refs)

    return kernel(
        body,
        (*hts, *pieces),
        [out] * 2,
        12,
        2 * rows * ff * width,
        scratch=(pltpu.VMEM((2, ff // 2, 2 * rows), F32), pltpu.VMEM((2 * rows, width), BF16)),
    )


def hidden_body(pieces, c0, c1, wd, slope, act, hid, gd, ud, comb0, comb1, gs):
    cw = jnp.concatenate([as_column(c0[...]), as_column(c1[...])], axis=0)
    for j, chunks in enumerate(pieces):
        at = 0
        for g in chunks:
            gs[pl.ds(j * PIECE, PIECE), pl.ds(at, g.shape[1])] = g[...]
            at += g.shape[1]
    tile = 256
    total = jnp.zeros((gs.shape[0], 1), F32)
    for f in range(wd.shape[0] // tile):
        at = pl.ds(f * tile, tile)
        back = nt(gs[...], wd[at, :])
        total = total + jnp.sum(hid[:, at].astype(F32) * back, axis=1, keepdims=True)
        back = cw * back
        gd[:, at] = (back * slope[:, at]).astype(BF16)
        ud[:, at] = (back * act[:, at]).astype(BF16)
    comb0[...] = as_row(total[:PIECE])
    comb1[...] = as_row(total[PIECE:])


def hidden_part(pieces, cws, wd, slope, act, hid):
    ff, d = wd.shape
    rows = 2 * PIECE
    counts = [len(chunks) for chunks in pieces]

    def body(*refs):
        first, second = refs[: counts[0]], refs[counts[0] : sum(counts)]
        hidden_body((first, second), *refs[sum(counts) :])

    return kernel(
        body,
        (*pieces[0], *pieces[1], *cws, wd, slope, act, hid),
        [((rows, ff), BF16), ((rows, ff), BF16), ROW, ROW],
        10,
        2 * rows * d * ff,
        scratch=(pltpu.VMEM((rows, d), BF16),),
    )


TILE = 256
EARLY = ((0, 0, 3), (1, 0, 3))
LATER = ((2, 0, 3), (3, 0, 3))
EXTRA = 128


def gate_body(first, specs, xta, xtb, gda, gdb, uda, udb, *refs):
    outs, mixed = refs[:-1], refs[-1]
    size = xta.shape[0] // BLOCKS // 2
    rows = xta.shape[1]
    chains = []
    for (p, low, high), out in zip(specs, outs):
        if p not in chains:
            chains.append(p)
            at = chains.index(p)
            for b in range(HALF):
                start = pl.multiple_of(block_at(ORDERS[p], first + b) * (2 * size) + (p % 2) * size, size)
                mixed[at, pl.ds(b * size, size), pl.ds(0, rows)] = xta[pl.ds(start, size), :]
                mixed[at, pl.ds(b * size, size), pl.ds(rows, rows)] = xtb[pl.ds(start, size), :]
        q = chains.index(p)
        ga, gb = (gda, gdb) if p < 2 else (uda, udb)
        per = TILE // LANES
        tall = size * per * (high - low)
        for n in range(low, high):
            at = pl.ds(n * TILE, TILE)
            part = nn(mixed[q, :, pl.ds(0, rows)], ga[:, at]) + nn(mixed[q, :, pl.ds(rows, rows)], gb[:, at])
            part = part.astype(BF16)
            for b in range(HALF):
                for k in range(per):
                    to = b * tall + ((n - low) * per + k) * size
                    out[pl.ds(to, size), :] = part[b * size : (b + 1) * size, k * LANES : (k + 1) * LANES]


def gate_half(first, specs, xts, gds, uds):
    d, rows = xts[0].shape
    tiles = [high - low for _, low, high in specs]
    outs = [((HALF * (d // BLOCKS // 2) * t * (TILE // LANES), LANES), BF16) for t in tiles]

    def body(*refs):
        gate_body(first, specs, *refs)

    return kernel(
        body,
        (*xts, *gds, *uds),
        outs,
        12,
        d * rows * TILE * sum(tiles),
        scratch=(pltpu.VMEM((len({p for p, _, _ in specs}), d // 4, 2 * rows), BF16),),
    )


def rows_body(gda, gdb, uda, udb, wg, wu, *refs):
    combs, (own, side, across, gd, ud) = refs[:4], refs[4:]
    half = gda.shape[0]
    for scratch, pair in ((gd, (gda, gdb)), (ud, (uda, udb))):
        for j, ref in enumerate(pair):
            scratch[pl.ds(j * half, half), :] = ref[...]
    places = ((own, 0), (side, 0), (across, 0), (side, PIECE))
    tile = 512
    for n in range(wg.shape[0] // tile):
        at = pl.ds(n * tile, tile)
        total = (nt(gd[...], wg[at, :]) + nt(ud[...], wu[at, :])).astype(BF16)
        for j, (out, row) in enumerate(places):
            out[pl.ds(row, PIECE), at] = total[j * PIECE : (j + 1) * PIECE, :]
    mine = lax.broadcasted_iota(jnp.int32, (PIECE, EXTRA), 1) == group_index()
    for comb, (out, row) in zip(combs, places):
        value = jnp.where(mine, as_column(comb[...]), 0.0)
        out[pl.ds(row, PIECE), pl.ds(wg.shape[0], EXTRA)] = value.astype(BF16)


def tokens_body(ids, own, side, across, grad, combine):
    total = own[...].astype(F32) + side[pl.ds(0, PIECE), :].astype(F32) + across[...].astype(F32)
    d = grad.shape[1]
    grad[...] = total[:, :d].astype(BF16)
    lanes = total[:, d:].T
    picked = jnp.zeros(combine.shape, F32)
    for e in range(4):
        picked = picked + jnp.where(ids[...] == e, lanes[e : e + 1, :], 0.0)
    combine[...] = picked


def finish_body(*refs):
    bases, last, (gate, up, down) = refs[:8], refs[8], refs[9:]
    half, low = gate.shape[0] // 2, down.shape[0]
    cols = down.shape[1] // 4
    received = last[...].astype(F32)
    done, at = [], 0
    for base in bases:
        done.append(base[...] + received[at : at + base.shape[0]])
        at += base.shape[0]
    for (p, first, _), total in zip(EARLY + LATER, done):
        out = gate if p < 2 else up
        for k in range(total.shape[0] // half):
            to = first * TILE + k * LANES
            out[pl.ds(p % 2 * half, half), pl.ds(to, LANES)] = total[k * half : (k + 1) * half].astype(BF16)
    for p, total in enumerate(done[4:]):
        for k in range(cols // LANES):
            down[:, pl.ds(p * cols + k * LANES, LANES)] = total[k * low : (k + 1) * low].astype(BF16)


def summed(arrays, start, stop, kind=BF16):
    total = 0.0
    for blocks, a in arrays:
        size = a.shape[0] // blocks
        total = total + a[start * size : stop * size].astype(F32)
    return total.astype(kind)


def shards(tokens, cotangent, expert_ids, combine, w_gate, w_up, w_down):
    wg, wu, wd = w_gate[0], w_up[0], w_down[0]
    d, ff = wg.shape
    rows = 4 * PIECE

    tok_far = moved(tokens, "zl", 1)
    tok_near = moved(tokens, "c", 1)
    own = kernel(route_body, (expert_ids.T, combine.T), [ROW] * 4, 2, 1 << 10)
    cws = [own[0]] + [moved(own[m], GROUP, m) for m in (1, 2, 3)]
    cwa, cwb = cws[:2], cws[2:]
    cot_near = moved(cotangent, "c", 1)
    cot_far = [moved(cotangent[:, k * d // 2 : (k + 1) * d // 2], "zl", 1) for k in range(2)]
    tok_both = moved(tok_far, "c", 1)
    cot_both = [moved(cot_far[k], "c", 1) for k in range(2)]

    fa = forward(tokens, tok_near, cwa, wg, wu)
    fb = forward(tok_far, tok_both, cwb, wg, wu)
    hts, xts = (fa[3], fb[3]), (fa[4], fb[4])
    pieces = [(cotangent, cot_near, cot_far[k], cot_both[k]) for k in range(2)]
    down_send = [a for k in range(2) for a in down_half(HALF, k, hts, pieces[k])]
    ha = hidden_part(((cotangent,), (cot_near,)), cwa, wd, *fa[:3])
    hb = hidden_part((cot_far, cot_both), cwb, wd, *fb[:3])
    gds, uds = (ha[0], hb[0]), (ha[1], hb[1])
    gate_send = list(gate_half(HALF, EARLY, xts, gds, uds))
    gate_send += gate_half(HALF, LATER, xts, gds, uds)
    down_keep = [a for k in range(2) for a in down_half(0, k, hts, pieces[k])]
    gate_keep = gate_half(0, EARLY + LATER, xts, gds, uds)
    own_rows, side_rows, far_rows = kernel(
        rows_body,
        (*gds, *uds, wg, wu, ha[2], ha[3], hb[2], hb[3]),
        [((n * PIECE, d + EXTRA), BF16) for n in (1, 2, 1)],
        12,
        4 * rows * d * ff,
        scratch=(pltpu.VMEM((rows, ff), BF16),) * 2,
    )

    down_got = [moved(down_send[p], *ORDERS[p][0]) for p in range(4)]
    gates, downs = [], [[(HALF, down_keep[p]), (HALF, down_got[p])] for p in range(4)]
    for spec, keep, send in zip(EARLY + LATER, gate_keep, gate_send):
        gates.append([(HALF, keep), (HALF, moved(send, *ORDERS[spec[0]][0]))])
    have = [[g for g, spec in zip(gates, EARLY + LATER) if spec[0] == p] + [downs[p]] for p in range(4)]
    left = {id(h): HALF for h in gates + downs}

    def exchange(held, step):
        sends = [summed(h, left[id(h)] // 2, left[id(h)]) for h in held]
        sent = jnp.concatenate(sends, axis=0)
        got = moved(sent, *step)
        at = 0
        for h, send in zip(held, sends):
            left[id(h)] //= 2
            h.append((left[id(h)], got[at : at + send.shape[0]]))
            at += send.shape[0]
        return got

    for p in (2, 3):
        exchange(downs[p : p + 1], ORDERS[p][1])
    for step in (1, 2, 3):
        for p in CHAINS:
            pieces = have[p][:1] if step == 1 and p > 1 else have[p]
            exchange(pieces, ORDERS[p][step])
    last = exchange(gates + downs, Z)
    bases = [summed(h[:-1], 0, 1, F32) for h in gates + downs]
    gate_grad, up_grad, down_grad = kernel(
        finish_body,
        (*bases, last),
        [((d // BLOCKS, ff), BF16), ((d // BLOCKS, ff), BF16), ((ff // BLOCKS, d), BF16)],
        4,
        1 << 20,
    )

    side_rows = moved(side_rows, "c", 1)
    far_rows = (far_rows.astype(F32) + side_rows[PIECE:].astype(F32)).astype(BF16)
    far_rows = moved(far_rows, "zl", 1)
    input_grad, combine_grad = kernel(
        tokens_body, (expert_ids.T, own_rows, side_rows, far_rows), [((PIECE, d), BF16), ((2, PIECE), F32)], 8, 1 << 20
    )
    combine_grad = combine_grad.T
    return (input_grad, combine_grad, gate_grad[None], up_grad[None], down_grad[None])


def solution(mesh):
    torus = Mesh(mesh.devices.reshape(4, 2, 4, 2, 2), EVERY)
    tokens, weights, grads = P(EVERY, None), P(GROUP, None, None), P(GROUP, REPLICA, None)

    return jax.shard_map(
        shards,
        mesh=torus,
        in_specs=(tokens, tokens, tokens, tokens, weights, weights, weights),
        out_specs=(tokens, tokens, grads, grads, grads),
        check_vma=False,
    )
```

```python
import jax
import jax.numpy as jnp
from jax import lax
from jax.experimental import pallas as pl
from jax.experimental.pallas import tpu as pltpu
from jax.sharding import Mesh
from jax.sharding import PartitionSpec as P


F32 = jnp.float32
BF16 = jnp.bfloat16
GROUP = ("zl", "c")
REPLICA = ("x", "zh", "y")
EVERY = ("x", "zh", "y", "zl", "c")
XA, XB, YA, YB, Z = ("x", 1), ("x", 3), ("y", 1), ("y", 3), ("zh", 1)
ORDERS = ((XA, XB, YA, YB, Z), (YA, YB, XA, XB, Z), (XB, XA, YB, YA, Z), (YB, YA, XB, XA, Z))
CHAINS = (0, 1, 2, 3)
BLOCKS = 32
HALF = BLOCKS // 2
PIECE = 128
LANES = 128
ROW = ((8, LANES), F32)


def moved(array, axis, mask):
    return lax.ppermute(array, axis, [(i, i ^ mask) for i in range(lax.axis_size(axis))])


def block_at(order, pos):
    masks = dict.fromkeys(REPLICA, 0)
    for step, (axis, mask) in enumerate(order):
        if pos >> (4 - step) & 1:
            masks[axis] ^= mask
    x, z, y = (lax.axis_index(axis) ^ masks[axis] for axis in REPLICA)
    return (x * 2 + z) * 4 + y


def group_index():
    return lax.axis_index("zl") * 2 + lax.axis_index("c")


def as_row(column):
    return jnp.broadcast_to(column, (column.shape[0], LANES)).T[:8]


def as_column(row):
    return jnp.broadcast_to(row[0:1, :], (LANES, LANES)).T[:, 0:1]


def nt(a, b):
    return lax.dot_general(a, b, (((1,), (1,)), ((), ())), preferred_element_type=F32)


def nn(a, b):
    return jnp.dot(a, b, preferred_element_type=F32)


def kernel(body, ins, outs, limit, flops, scratch=()):
    vmem = pl.BlockSpec(memory_space=pltpu.VMEM)
    return pl.pallas_call(
        body,
        in_specs=[vmem] * len(ins),
        out_specs=[vmem] * len(outs),
        out_shape=[jax.ShapeDtypeStruct(s, t) for s, t in outs],
        scratch_shapes=list(scratch),
        compiler_params=pltpu.CompilerParams(vmem_limit_bytes=limit << 20),
        cost_estimate=pl.CostEstimate(flops=flops, transcendentals=0, bytes_accessed=1 << 20),
    )(*ins)


def route_body(ids, combine, *outs):
    mine = group_index()
    for m, out in enumerate(outs):
        chosen = ids[...] == (mine ^ m)
        row = jnp.sum(jnp.where(chosen, combine[...], 0.0), axis=0, keepdims=True)
        out[...] = jnp.broadcast_to(row, out.shape)


def forward_body(x0, x1, c0, c1, wg, wu, slope, act_out, hid, cht, xt, xs):
    cw = jnp.concatenate([as_column(c0[...]), as_column(c1[...])], axis=0)
    for j, x in enumerate((x0, x1)):
        xs[pl.ds(j * PIECE, PIECE), :] = x[...]
    tile = 256
    for f in range(wg.shape[1] // tile):
        at = pl.ds(f * tile, tile)
        gate = nn(xs[...], wg[:, at])
        up = nn(xs[...], wu[:, at])
        sig = jax.nn.sigmoid(gate)
        act = gate * sig
        slope[:, at] = up * (sig * (1.0 + gate * (1.0 - sig)))
        act_out[:, at] = act
        hidden = act * up
        hid[:, at] = hidden.astype(BF16)
        cht[at, :] = (cw * hidden).T
    for j in range(2):
        xt[:, pl.ds(j * PIECE, PIECE)] = xs[pl.ds(j * PIECE, PIECE), :].T


def forward(x0, x1, cws, wg, wu):
    d, ff = wg.shape
    rows = 2 * PIECE
    outs = [((rows, ff), F32), ((rows, ff), F32), ((rows, ff), BF16), ((ff, rows), F32), ((d, rows), BF16)]
    return kernel(
        forward_body, (x0, x1, *cws, wg, wu), outs, 12, 4 * rows * d * ff, scratch=(pltpu.VMEM((rows, d), BF16),)
    )


def down_body(first, chunk, hta, htb, g0, g1, g2, g3, *refs):
    outs, (mixed, gs) = refs[:-2], refs[-2:]
    cols = g2.shape[1] // 2
    for j, g in enumerate((g0, g1)):
        gs[pl.ds(j * PIECE, PIECE), :] = g[:, pl.ds(chunk * 2 * cols, 2 * cols)]
    for j, g in enumerate((g2, g3)):
        gs[pl.ds((2 + j) * PIECE, PIECE), :] = g[...]
    size = hta.shape[0] // BLOCKS
    rows = hta.shape[1]
    for q in range(2):
        out = outs[q]
        for b in range(HALF):
            start = pl.multiple_of(block_at(ORDERS[2 * chunk + q], first + b) * size, 8)
            mixed[q, pl.ds(b * size, size), pl.ds(0, rows)] = hta[pl.ds(start, size), :]
            mixed[q, pl.ds(b * size, size), pl.ds(rows, rows)] = htb[pl.ds(start, size), :]
        part = nn(mixed[q].astype(BF16), gs[:, pl.ds(q * cols, cols)])
        for b in range(HALF):
            block = part[b * size : (b + 1) * size]
            stack = [block[:, k * LANES : (k + 1) * LANES] for k in range(cols // LANES)]
            tall = size * len(stack)
            out[pl.ds(b * tall, tall), :] = jnp.concatenate(stack, axis=0).astype(BF16)


def down_half(first, chunk, hts, pieces):
    ff, rows = hts[0].shape
    width = pieces[2].shape[1]
    out = ((HALF * ff // BLOCKS * (width // 2 // LANES), LANES), BF16)

    def body(*refs):
        down_body(first, chunk, *refs)

    return kernel(
        body,
        (*hts, *pieces),
        [out] * 2,
        12,
        2 * rows * ff * width,
        scratch=(pltpu.VMEM((2, ff // 2, 2 * rows), F32), pltpu.VMEM((2 * rows, width), BF16)),
    )


def hidden_body(pieces, c0, c1, wd, slope, act, hid, gd, ud, comb0, comb1, gs):
    cw = jnp.concatenate([as_column(c0[...]), as_column(c1[...])], axis=0)
    for j, chunks in enumerate(pieces):
        at = 0
        for g in chunks:
            gs[pl.ds(j * PIECE, PIECE), pl.ds(at, g.shape[1])] = g[...]
            at += g.shape[1]
    tile = 256
    total = jnp.zeros((gs.shape[0], 1), F32)
    for f in range(wd.shape[0] // tile):
        at = pl.ds(f * tile, tile)
        back = nt(gs[...], wd[at, :])
        total = total + jnp.sum(hid[:, at].astype(F32) * back, axis=1, keepdims=True)
        back = cw * back
        gd[:, at] = (back * slope[:, at]).astype(BF16)
        ud[:, at] = (back * act[:, at]).astype(BF16)
    comb0[...] = as_row(total[:PIECE])
    comb1[...] = as_row(total[PIECE:])


def hidden_part(pieces, cws, wd, slope, act, hid):
    ff, d = wd.shape
    rows = 2 * PIECE
    counts = [len(chunks) for chunks in pieces]

    def body(*refs):
        first, second = refs[: counts[0]], refs[counts[0] : sum(counts)]
        hidden_body((first, second), *refs[sum(counts) :])

    return kernel(
        body,
        (*pieces[0], *pieces[1], *cws, wd, slope, act, hid),
        [((rows, ff), BF16), ((rows, ff), BF16), ROW, ROW],
        10,
        2 * rows * d * ff,
        scratch=(pltpu.VMEM((rows, d), BF16),),
    )


TILE = 256
EARLY = ((0, 0, 3), (1, 0, 3))
LATER = ((2, 0, 3), (3, 0, 3))
EXTRA = 128


def gate_body(first, specs, xta, xtb, gda, gdb, uda, udb, *refs):
    outs, mixed = refs[:-1], refs[-1]
    size = xta.shape[0] // BLOCKS // 2
    rows = xta.shape[1]
    chains = []
    for (p, low, high), out in zip(specs, outs):
        if p not in chains:
            chains.append(p)
            at = chains.index(p)
            for b in range(HALF):
                start = pl.multiple_of(block_at(ORDERS[p], first + b) * (2 * size) + (p % 2) * size, size)
                mixed[at, pl.ds(b * size, size), pl.ds(0, rows)] = xta[pl.ds(start, size), :]
                mixed[at, pl.ds(b * size, size), pl.ds(rows, rows)] = xtb[pl.ds(start, size), :]
        q = chains.index(p)
        ga, gb = (gda, gdb) if p < 2 else (uda, udb)
        per = TILE // LANES
        tall = size * per * (high - low)
        for n in range(low, high):
            at = pl.ds(n * TILE, TILE)
            part = nn(mixed[q, :, pl.ds(0, rows)], ga[:, at]) + nn(mixed[q, :, pl.ds(rows, rows)], gb[:, at])
            part = part.astype(BF16)
            for b in range(HALF):
                for k in range(per):
                    to = b * tall + ((n - low) * per + k) * size
                    out[pl.ds(to, size), :] = part[b * size : (b + 1) * size, k * LANES : (k + 1) * LANES]


def gate_half(first, specs, xts, gds, uds):
    d, rows = xts[0].shape
    tiles = [high - low for _, low, high in specs]
    outs = [((HALF * (d // BLOCKS // 2) * t * (TILE // LANES), LANES), BF16) for t in tiles]

    def body(*refs):
        gate_body(first, specs, *refs)

    return kernel(
        body,
        (*xts, *gds, *uds),
        outs,
        12,
        d * rows * TILE * sum(tiles),
        scratch=(pltpu.VMEM((len({p for p, _, _ in specs}), d // 4, 2 * rows), BF16),),
    )


def rows_body(gda, gdb, uda, udb, wg, wu, *refs):
    combs, (own, side, across, gd, ud) = refs[:4], refs[4:]
    half = gda.shape[0]
    for scratch, pair in ((gd, (gda, gdb)), (ud, (uda, udb))):
        for j, ref in enumerate(pair):
            scratch[pl.ds(j * half, half), :] = ref[...]
    places = ((own, 0), (side, 0), (across, 0), (side, PIECE))
    tile = 512
    for n in range(wg.shape[0] // tile):
        at = pl.ds(n * tile, tile)
        total = (nt(gd[...], wg[at, :]) + nt(ud[...], wu[at, :])).astype(BF16)
        for j, (out, row) in enumerate(places):
            out[pl.ds(row, PIECE), at] = total[j * PIECE : (j + 1) * PIECE, :]
    mine = lax.broadcasted_iota(jnp.int32, (PIECE, EXTRA), 1) == group_index()
    for comb, (out, row) in zip(combs, places):
        value = jnp.where(mine, as_column(comb[...]), 0.0)
        out[pl.ds(row, PIECE), pl.ds(wg.shape[0], EXTRA)] = value.astype(BF16)


def tokens_body(ids, own, side, across, grad, combine):
    total = own[...].astype(F32) + side[pl.ds(0, PIECE), :].astype(F32) + across[...].astype(F32)
    d = grad.shape[1]
    grad[...] = total[:, :d].astype(BF16)
    lanes = total[:, d:].T
    picked = jnp.zeros(combine.shape, F32)
    for e in range(4):
        picked = picked + jnp.where(ids[...] == e, lanes[e : e + 1, :], 0.0)
    combine[...] = picked


def finish_body(*refs):
    bases, lasts, (gate, up, down) = refs[:8], refs[8:10], refs[10:]
    half, low = gate.shape[0] // 2, down.shape[0]
    cols = down.shape[1] // 4
    received = [r[...].astype(F32) for r in lasts]
    done, at = [], [0, 0]
    for n, base in enumerate(bases):
        k = n % 4 // 2
        done.append(base[...] + received[k][at[k] : at[k] + base.shape[0]])
        at[k] += base.shape[0]
    for (p, first, _), total in zip(EARLY + LATER, done):
        out = gate if p < 2 else up
        for k in range(total.shape[0] // half):
            to = first * TILE + k * LANES
            out[pl.ds(p % 2 * half, half), pl.ds(to, LANES)] = total[k * half : (k + 1) * half].astype(BF16)
    for p, total in enumerate(done[4:]):
        for k in range(cols // LANES):
            down[:, pl.ds(p * cols + k * LANES, LANES)] = total[k * low : (k + 1) * low].astype(BF16)


def summed(arrays, start, stop, kind=BF16):
    total = 0.0
    for blocks, a in arrays:
        size = a.shape[0] // blocks
        total = total + a[start * size : stop * size].astype(F32)
    return total.astype(kind)


def shards(tokens, cotangent, expert_ids, combine, w_gate, w_up, w_down):
    wg, wu, wd = w_gate[0], w_up[0], w_down[0]
    d, ff = wg.shape
    rows = 4 * PIECE

    tok_far = moved(tokens, "zl", 1)
    tok_near = moved(tokens, "c", 1)
    own = kernel(route_body, (expert_ids.T, combine.T), [ROW] * 4, 2, 1 << 10)
    cws = [own[0]] + [moved(own[m], GROUP, m) for m in (1, 2, 3)]
    cwa, cwb = cws[:2], cws[2:]
    cot_near = moved(cotangent, "c", 1)
    cot_far = [moved(cotangent[:, k * d // 2 : (k + 1) * d // 2], "zl", 1) for k in range(2)]
    tok_both = moved(tok_far, "c", 1)
    cot_both = [moved(cot_far[k], "c", 1) for k in range(2)]

    fa = forward(tokens, tok_near, cwa, wg, wu)
    fb = forward(tok_far, tok_both, cwb, wg, wu)
    hts, xts = (fa[3], fb[3]), (fa[4], fb[4])
    pieces = [(cotangent, cot_near, cot_far[k], cot_both[k]) for k in range(2)]
    down_send = [a for k in range(2) for a in down_half(HALF, k, hts, pieces[k])]
    ha = hidden_part(((cotangent,), (cot_near,)), cwa, wd, *fa[:3])
    hb = hidden_part((cot_far, cot_both), cwb, wd, *fb[:3])
    gds, uds = (ha[0], hb[0]), (ha[1], hb[1])
    gate_send = list(gate_half(HALF, EARLY, xts, gds, uds))
    gate_send += gate_half(HALF, LATER, xts, gds, uds)
    down_keep = [a for k in range(2) for a in down_half(0, k, hts, pieces[k])]
    gate_keep = gate_half(0, EARLY + LATER, xts, gds, uds)
    own_rows, side_rows, far_rows = kernel(
        rows_body,
        (*gds, *uds, wg, wu, ha[2], ha[3], hb[2], hb[3]),
        [((n * PIECE, d + EXTRA), BF16) for n in (1, 2, 1)],
        12,
        4 * rows * d * ff,
        scratch=(pltpu.VMEM((rows, ff), BF16),) * 2,
    )

    down_got = [moved(down_send[p], *ORDERS[p][0]) for p in range(4)]
    gates, downs = [], [[(HALF, down_keep[p]), (HALF, down_got[p])] for p in range(4)]
    for spec, keep, send in zip(EARLY + LATER, gate_keep, gate_send):
        gates.append([(HALF, keep), (HALF, moved(send, *ORDERS[spec[0]][0]))])
    have = [[g for g, spec in zip(gates, EARLY + LATER) if spec[0] == p] + [downs[p]] for p in range(4)]
    left = {id(h): HALF for h in gates + downs}

    def exchange(held, step):
        sends = [summed(h, left[id(h)] // 2, left[id(h)]) for h in held]
        sent = jnp.concatenate(sends, axis=0)
        got = moved(sent, *step)
        at = 0
        for h, send in zip(held, sends):
            left[id(h)] //= 2
            h.append((left[id(h)], got[at : at + send.shape[0]]))
            at += send.shape[0]
        return got

    for step in (1, 2, 3):
        for p in CHAINS:
            exchange(have[p], ORDERS[p][step])
    last_a = exchange(gates[:2] + downs[:2], Z)
    last_b = exchange(gates[2:] + downs[2:], Z)
    bases = [summed(h[:-1], 0, 1, F32) for h in gates + downs]
    gate_grad, up_grad, down_grad = kernel(
        finish_body,
        (*bases, last_a, last_b),
        [((d // BLOCKS, ff), BF16), ((d // BLOCKS, ff), BF16), ((ff // BLOCKS, d), BF16)],
        4,
        1 << 20,
    )

    side_rows = moved(side_rows, "c", 1)
    far_rows = (far_rows.astype(F32) + side_rows[PIECE:].astype(F32)).astype(BF16)
    far_rows = moved(far_rows, "zl", 1)
    input_grad, combine_grad = kernel(
        tokens_body, (expert_ids.T, own_rows, side_rows, far_rows), [((PIECE, d), BF16), ((2, PIECE), F32)], 8, 1 << 20
    )
    combine_grad = combine_grad.T
    return (input_grad, combine_grad, gate_grad[None], up_grad[None], down_grad[None])


def solution(mesh):
    torus = Mesh(mesh.devices.reshape(4, 2, 4, 2, 2), EVERY)
    tokens, weights, grads = P(EVERY, None), P(GROUP, None, None), P(GROUP, REPLICA, None)

    return jax.shard_map(
        shards,
        mesh=torus,
        in_specs=(tokens, tokens, tokens, tokens, weights, weights, weights),
        out_specs=(tokens, tokens, grads, grads, grads),
        check_vma=False,
    )
```
